32 devices in a mesh: patch: 8 (over z, y), hidden: 4 (over x, core).
Axes of the slice: x: 2, y: 2, z: 4, core: 2. Of those that a mesh axis runs over, the one named last changes fastest.
Arguments:
- grid_latent: bfloat16 [24576, 512], P('patch'), may hold values from -6 to 6
- mesh_latent: bfloat16 [40960, 512], P('patch'), may hold values from -6 to 6
- edge_latent: bfloat16 [65536, 512], P('patch'), may hold values from -6 to 6
- senders: int32 [65536], P('patch'), may hold values from 0 to 24575, as said below
- receivers: int32 [65536], P('patch'), may hold values from 0 to 40959
- mesh_slot: int32 [40960], replicated, may hold values from 0 to 40959, as said below
- edge_counts: int32 [8], P('patch'), may hold values from 2730 to 8192, as said below
- w_edge: bfloat16 [512, 512], P(None, 'hidden'), may hold values from -0.25 to 0.25
- w_sender: bfloat16 [512, 512], P(None, 'hidden'), may hold values from -0.25 to 0.25
- w_receiver: bfloat16 [512, 512], P(None, 'hidden'), may hold values from -0.25 to 0.25
- edge_bias: float32 [512], P('hidden'), may hold values from -3 to 3
- w_edge_out: bfloat16 [512, 512], P('hidden'), may hold values from -0.25 to 0.25
- edge_out_bias: float32 [512], P('hidden'), may hold values from -3 to 3
- edge_gain: float32 [512], P('hidden'), may hold values from 0.25 to 1.75
- edge_shift: float32 [512], P('hidden'), may hold values from -2 to 2
- w_mesh_in: bfloat16 [512, 512], P(None, 'hidden'), may hold values from -0.25 to 0.25
- w_message_in: bfloat16 [512, 512], P(None, 'hidden'), may hold values from -0.25 to 0.25
- mesh_bias: float32 [512], P('hidden'), may hold values from -3 to 3
- w_mesh_out: bfloat16 [512, 512], P('hidden'), may hold values from -0.25 to 0.25
- mesh_out_bias: float32 [512], P('hidden'), may hold values from -3 to 3
- mesh_gain: float32 [512], P('hidden'), may hold values from 0.25 to 1.75
- mesh_shift: float32 [512], P('hidden'), may hold values from -2 to 2
Outputs:
- mesh_out: bfloat16 [40960, 512], P('patch', 'hidden')
- edge_out: bfloat16 [65536, 512], P('patch', 'hidden')
The draws below stay inside these ranges and needn't reach their ends.
Inputs may be any that keep to these rules, and one draw needn't show every extreme that they name: `mesh_slot`: A permutation of the mesh node ids 0 to 40959; owner block p holds mesh rows p * 5120 to (p + 1) * 5120 - 1. `senders`: edge slots of block p (slots p * 8192 to (p + 1) * 8192 - 1) send from grid nodes p * 3072 to (p + 1) * 3072 - 1. Only the first edge_counts[p] slots of block p are live; some block is full.
All inputs are finite; a program needn't handle non-finite values.
Results may differ from the reference program's by a relative error of at most 0.014.
Values may be sent and summed in bfloat16 or wider, within the bound.
A program may use at most 192 MiB of HBM per device.

```python
import jax
import jax.numpy as jnp
from jax import lax

LATENT = 512
G_DEV = 3072
E_DEV = 8192
MESH_DEV = 5120
GRID = 24576
EDGES = 65536
MESH = 40960
N_HIDDEN = 4


def mesh_order(key):
    return jax.random.permutation(jax.random.fold_in(key, 11), MESH).astype(jnp.int32)


def draw_mesh_slot(key, part):
    return mesh_order(key)


def draw_receivers(key, part):
    order = mesh_order(key)
    inverse = jnp.argsort(order, stable=True).astype(jnp.int32)
    first, second = jax.random.split(jax.random.fold_in(key, 12))
    third = jax.random.fold_in(key, 15)
    position = jnp.arange(EDGES, dtype=jnp.int32)
    blocks = EDGES // E_DEV
    pick = jax.random.randint(first, (EDGES,), 0, 8)
    anywhere = jax.random.randint(third, (EDGES,), 0, blocks).astype(jnp.int32)
    offset = jnp.where(pick == 4, -1, jnp.where(pick == 7, 1, 0)).astype(jnp.int32)
    nearby = (position // E_DEV + offset + blocks) % blocks
    owner = jnp.where(pick < 4, anywhere, nearby).astype(jnp.int32)
    target = owner * MESH_DEV + jax.random.randint(second, (EDGES,), 0, MESH_DEV)
    return jnp.take(inverse, target).astype(jnp.int32)


def draw_senders(key, part):
    position = jnp.arange(EDGES, dtype=jnp.int32)
    local = jax.random.randint(jax.random.fold_in(key, 13), (EDGES,), 0, G_DEV)
    return (position // E_DEV * G_DEV + local).astype(jnp.int32)


def draw_edge_counts(key, part):
    first, second = jax.random.split(jax.random.fold_in(key, 14))
    blocks = EDGES // E_DEV
    counts = jax.random.randint(first, (blocks,), E_DEV // 3, E_DEV + 1)
    fullest = jax.random.randint(second, (), 0, blocks)
    return jnp.where(jnp.arange(blocks) == fullest, E_DEV, counts).astype(jnp.int32)


def steps_of(own_key, extent, shards, smallest, high):
    level, own = 1.0, jax.random.fold_in(own_key, 6)
    for axis_at, shards_of in shards:
        heights = jnp.exp(jax.random.uniform(jax.random.fold_in(own, axis_at), (shards_of,), jnp.float32, smallest / len(shards), high / len(shards)))
        level = level * jnp.repeat(heights, extent[axis_at] // shards_of).reshape([-1 if axis == axis_at else 1 for axis in range(len(extent))])
    return level


def bell_draw(rng, extent, scale, most, shards=(), held_as=jnp.bfloat16):
    entries = scale * jax.random.normal(rng, extent, jnp.float32)
    if shards:
        entries = entries * steps_of(rng, extent, shards, -0.22, 0.18)
    return jnp.clip(entries, -most, most).astype(held_as)


def setup_inputs(seed: int = 0) -> dict:
    key_list = jax.random.split(jax.random.key(seed), 23)
    return {
        "grid_latent": bell_draw(key_list[0], (GRID, LATENT), 1.0, 6.0, ((0, 8),)),
        "mesh_latent": bell_draw(key_list[1], (MESH, LATENT), 1.0, 6.0, ((0, 8),)),
        "edge_latent": bell_draw(key_list[2], (EDGES, LATENT), 1.0, 6.0, ((0, 8),)),
        "senders": draw_senders(jax.random.fold_in(key_list[22], 71), 0),
        "receivers": draw_receivers(jax.random.fold_in(key_list[22], 71), 0),
        "mesh_slot": draw_mesh_slot(jax.random.fold_in(key_list[22], 71), 0),
        "edge_counts": draw_edge_counts(jax.random.fold_in(key_list[22], 71), 0),
        "w_edge": bell_draw(key_list[7], (LATENT, LATENT), LATENT ** -0.5, 0.25, ((1, 4),)),
        "w_sender": bell_draw(key_list[8], (LATENT, LATENT), LATENT ** -0.5, 0.25, ((1, 4),)),
        "w_receiver": bell_draw(key_list[9], (LATENT, LATENT), LATENT ** -0.5, 0.25, ((1, 4),)),
        "edge_bias": bell_draw(key_list[10], (LATENT,), 0.5, 3.0, ((0, 4),), jnp.float32),
        "w_edge_out": bell_draw(key_list[11], (LATENT, LATENT), LATENT ** -0.5, 0.25, ((0, 4),)),
        "edge_out_bias": bell_draw(key_list[12], (LATENT,), 0.5, 3.0, ((0, 4),), jnp.float32),
        "edge_gain": jnp.clip(1.0 + 0.15 * jax.random.normal(key_list[13], (LATENT,), jnp.float32), 0.25, 1.75),
        "edge_shift": bell_draw(key_list[14], (LATENT,), 0.3, 2.0, ((0, 4),), jnp.float32),
        "w_mesh_in": bell_draw(key_list[15], (LATENT, LATENT), LATENT ** -0.5, 0.25, ((1, 4),)),
        "w_message_in": bell_draw(key_list[16], (LATENT, LATENT), LATENT ** -0.5, 0.25, ((1, 4),)),
        "mesh_bias": bell_draw(key_list[17], (LATENT,), 0.5, 3.0, ((0, 4),), jnp.float32),
        "w_mesh_out": bell_draw(key_list[18], (LATENT, LATENT), LATENT ** -0.5, 0.25, ((0, 4),)),
        "mesh_out_bias": bell_draw(key_list[19], (LATENT,), 0.5, 3.0, ((0, 4),), jnp.float32),
        "mesh_gain": jnp.clip(1.0 + 0.15 * jax.random.normal(key_list[20], (LATENT,), jnp.float32), 0.25, 1.75),
        "mesh_shift": bell_draw(key_list[21], (LATENT,), 0.3, 2.0, ((0, 4),), jnp.float32),
    }


def group_sum(hidden_units, w_out):
    width = w_out.shape[0] // N_HIDDEN
    total = jnp.zeros((hidden_units.shape[0], w_out.shape[1]), jnp.float32)
    for group in range(N_HIDDEN):
        part = jnp.dot(hidden_units[:, group * width:(group + 1) * width], w_out[group * width:(group + 1) * width], preferred_element_type=jnp.float32)
        part = lax.optimization_barrier(part.astype(jnp.bfloat16))
        total = total + part.astype(jnp.float32)
    return total

def normalize(values, gain, offset):
    center = lax.optimization_barrier(jnp.mean(values, axis=1, keepdims=True))
    centered = values - center
    spread = lax.optimization_barrier(jnp.mean(centered * centered, axis=1, keepdims=True))
    return centered * lax.rsqrt(spread + 1e-05) * gain + offset

def reference(grid_latent, mesh_latent, edge_latent, senders, receivers, mesh_slot, edge_counts, w_edge, w_sender, w_receiver, edge_bias, w_edge_out, edge_out_bias, edge_gain, edge_shift, w_mesh_in, w_message_in, mesh_bias, w_mesh_out, mesh_out_bias, mesh_gain, mesh_shift):
    target = jnp.take(mesh_slot, receivers).astype(jnp.int32)
    position = jnp.arange(EDGES, dtype=jnp.int32)
    live = (position % E_DEV < jnp.take(edge_counts, position // E_DEV)).astype(jnp.float32)
    receiver_proj = jnp.dot(mesh_latent, w_receiver, preferred_element_type=jnp.float32).astype(jnp.bfloat16)
    sender_proj = jnp.dot(grid_latent, w_sender, preferred_element_type=jnp.float32)
    edge_pre = jnp.dot(edge_latent, w_edge, preferred_element_type=jnp.float32)
    edge_pre = edge_pre + jnp.take(sender_proj, senders, axis=0) + jnp.take(receiver_proj, target, axis=0).astype(jnp.float32) + edge_bias
    edge_hidden = jax.nn.silu(edge_pre).astype(jnp.bfloat16)
    edge_sum = group_sum(edge_hidden, w_edge_out) + edge_out_bias
    message = normalize(edge_sum, edge_gain, edge_shift) * live[:, None]
    edge_out = (edge_latent.astype(jnp.float32) + message).astype(jnp.bfloat16)
    summed = jax.ops.segment_sum(message, target, num_segments=MESH).astype(jnp.bfloat16)
    mesh_pre = jnp.dot(mesh_latent, w_mesh_in, preferred_element_type=jnp.float32) + jnp.dot(summed, w_message_in, preferred_element_type=jnp.float32) + mesh_bias
    mesh_hidden = jax.nn.silu(mesh_pre).astype(jnp.bfloat16)
    mesh_sum = group_sum(mesh_hidden, w_mesh_out) + mesh_out_bias
    mesh_out = (mesh_latent.astype(jnp.float32) + normalize(mesh_sum, mesh_gain, mesh_shift)).astype(jnp.bfloat16)
    return (mesh_out, edge_out)
```

```python
import functools

import jax
import jax.numpy as jnp
from jax import lax
from jax.experimental import pallas as pl
from jax.experimental.pallas import tpu as pltpu
from jax.sharding import PartitionSpec as P

EPSILON = 1e-05
CHUNK = 256
OWN_CHUNKS = 3
NEAR_CHUNKS = 2
FAR_ROWS = 192
CLASS_ROWS = 8


def iota(shape, axis):
    return lax.broadcasted_iota(jnp.int32, shape, axis)


def one_hot(cond):
    return jnp.where(cond, 1.0, 0.0).astype(jnp.bfloat16)


def dot(a, b):
    return jnp.dot(a, b, preferred_element_type=jnp.float32)


def dot_nt(a, b):
    return lax.dot_general(a, b, (((1,), (1,)), ((), ())), preferred_element_type=jnp.float32)


def wide(block):
    return jnp.concatenate([block[j : j + 1, :] for j in range(block.shape[0])], axis=1)


def normalize(total, gain, offset):
    width = total.shape[1]
    center = jnp.sum(total, axis=1, keepdims=True) / width
    centered = total - center
    spread = jnp.sum(centered * centered, axis=1, keepdims=True) / width
    return centered * lax.rsqrt(spread + EPSILON) * gain + offset


def class_plan(patches):
    starts = [0, OWN_CHUNKS] + [OWN_CHUNKS + 2 * NEAR_CHUNKS + k - 2 for k in range(2, patches - 1)]
    starts.append(OWN_CHUNKS + NEAR_CHUNKS)
    caps = [OWN_CHUNKS * CHUNK, NEAR_CHUNKS * CHUNK] + [FAR_ROWS] * (patches - 3) + [NEAR_CHUNKS * CHUNK]
    return starts, caps, OWN_CHUNKS + 2 * NEAR_CHUNKS + patches - 3


def index_kernel(sizes, where_am_i, recv_ref, send_ref, table_ref, req_ref, edge_ref, send_out_ref, where_ref, target, masks, position, local, totals):
    patches, ranks, mesh_rows, parts = sizes
    groups = recv_ref.shape[0]
    own_rows = mesh_rows // ranks
    starts, caps, chunks = class_plan(patches)
    high = table_ref.shape[1]
    me, rank_me, count = where_am_i[0], where_am_i[1], where_am_i[2]

    def lookup(i, carry):
        row = wide(recv_ref[pl.ds(i * 8, 8), :])
        hot = one_hot(iota((high, 1024), 0) == (row >> 7))
        found = dot(table_ref[...], hot)
        low = iota((128, 1024), 0) == (row & 127)
        value = jnp.zeros((1, 1024), jnp.float32)
        for part in range(parts):
            piece = jnp.where(low, found[part * 128 : (part + 1) * 128], 0.0)
            value = value + float(256**part) * jnp.sum(piece, axis=0, keepdims=True)
        value = value.astype(jnp.int32)
        block = jnp.concatenate([value[:, j * 128 : (j + 1) * 128] for j in range(8)], axis=0)
        target[pl.ds(i * 8, 8), :] = block
        return carry

    lax.fori_loop(0, groups // 8, lookup, 0)

    shape = (groups, 128)
    goal = target[...]
    owner = sum((goal >= k * mesh_rows).astype(jnp.int32) for k in range(1, patches))
    inside = goal - owner * mesh_rows
    part = sum((inside >= k * own_rows).astype(jnp.int32) for k in range(1, ranks))
    offset = owner - me
    offset = jnp.where(offset < 0, offset + patches, offset)
    slot = iota(shape, 0) * 128 + iota(shape, 1)
    live = slot < count
    label = jnp.where(live, offset * ranks + part, -1)
    classes = patches * ranks
    for c in range(classes):
        masks[c * groups : (c + 1) * groups, :] = one_hot(label == c)
    steps = jnp.concatenate([one_hot(iota((128, 128), 0) <= iota((128, 128), 1)), jnp.ones((128, 128), jnp.bfloat16)], axis=1)
    totals[...] = dot(masks[...], steps)
    below = one_hot(iota((groups, groups), 1) < iota((groups, groups), 0))
    rank = jnp.zeros(shape, jnp.float32)
    over = jnp.zeros((1, 128), jnp.float32)
    for c in range(classes):
        block = totals[c * groups : (c + 1) * groups, :]
        inner, whole = block[:, :128], block[:, 128:]
        before = dot(below, whole.astype(jnp.bfloat16))
        mine = jnp.where(label == c, 1.0, 0.0)
        rank = rank + mine * (inner - 1.0 + before)
        full = before[groups - 1 :, :] + whole[groups - 1 :, :]
        over = jnp.maximum(over, jnp.where(full > float(caps[c // ranks]), 1.0, 0.0))
    rank = rank.astype(jnp.int32)
    first = jnp.zeros(shape, jnp.int32)
    cap = jnp.zeros(shape, jnp.int32)
    for k in range(patches):
        first = jnp.where(offset == k, starts[k] * CHUNK, first)
        cap = jnp.where(offset == k, caps[k], cap)
    spot = part * (chunks * CHUNK) + first + rank
    spot = jnp.minimum(spot, ranks * chunks * CHUNK - 1)
    where_ref[...] = jnp.where(live, spot, 0)
    mine = live & (part == rank_me) & (rank < cap)
    position[...] = jnp.where(mine, offset * (CLASS_ROWS * 128) + rank, -1)
    local[...] = inside - rank_me * own_rows

    rows = patches * CLASS_ROWS

    def invert(i, total):
        at = pl.ds(i * 8, 8)
        spots = wide(position[at, :])
        edge = i * 1024 + iota((1, 1024), 1)
        line = wide(local[at, :])
        sender = wide(send_ref[at, :])
        here = iota((rows, 1024), 0) == (spots >> 7)
        values = [jnp.ones((1, 1024), jnp.int32)]
        for value in (line, edge, sender):
            values += [value >> 8, value & 255]
        left = jnp.concatenate(
            [jnp.where(here, value.astype(jnp.float32), 0.0).astype(jnp.bfloat16) for value in values], axis=0
        )
        right = one_hot(iota((128, 1024), 0) == (spots & 127))
        return total + dot_nt(left, right)

    total = lax.fori_loop(0, groups // 8, invert, jnp.zeros((7 * rows, 128), jnp.float32))
    filled = total[:rows] > 0.5

    def value_of(n):
        value = total[n * rows : (n + 1) * rows] * 256.0 + total[(n + 1) * rows : (n + 2) * rows]
        return jnp.where(filled, value, -1.0).astype(jnp.int32)

    last = (iota((rows, 128), 0) & (CLASS_ROWS - 1)) == CLASS_ROWS - 1
    req_ref[...] = jnp.where(last, over.astype(jnp.int32), value_of(1))
    edge_ref[...] = value_of(3)
    send_out_ref[...] = value_of(5)


def plan_edges(here, receivers, sender_local, mesh_slot, patches, ranks, mesh_rows):
    groups = receivers.shape[0] // 128
    mesh_total = mesh_slot.shape[0]
    high = mesh_total // 128
    parts = 1
    while 256**parts < mesh_total:
        parts += 1
    turned = mesh_slot.reshape(high, 128).T
    table = jnp.concatenate([((turned >> (8 * i)) & 255).astype(jnp.bfloat16) for i in range(parts)], 0)
    rows = patches * CLASS_ROWS
    vmem = pl.BlockSpec(memory_space=pltpu.VMEM)
    lists = jax.ShapeDtypeStruct((rows, 128), jnp.int32)
    return pl.pallas_call(
        functools.partial(index_kernel, (patches, ranks, mesh_rows, parts)),
        in_specs=[pl.BlockSpec(memory_space=pltpu.SMEM), vmem, vmem, vmem],
        out_specs=[vmem] * 4,
        out_shape=[lists, lists, lists, jax.ShapeDtypeStruct((groups, 128), jnp.int32)],
        scratch_shapes=[
            pltpu.VMEM((groups, 128), jnp.int32),
            pltpu.VMEM((patches * ranks * groups, 128), jnp.bfloat16),
            pltpu.VMEM((groups, 128), jnp.int32),
            pltpu.VMEM((groups, 128), jnp.int32),
            pltpu.VMEM((patches * ranks * groups, 256), jnp.float32),
        ],
        name="plan_edges",
    )(here, receivers.reshape(groups, 128), sender_local.reshape(groups, 128), table)


def stage_kernel(sizes, count, where, req, edges, sends, vector, w_edge, w_sender, w_receiver, w_edge_out, w_mesh_in, w_message_in, w_mesh_out, mesh, edge, grid, mesh_out, edge_out, flag, mesh_v, edge_v, grid_v, first_w, second_w, third_w, fourth_w, vectors, reqs, rows_out, rows_in, picked_e, picked_s, messages, outgoing, incoming, table, staged, finished, finished_mesh, local_sem, weight_send, weight_recv, req_send, req_recv, row_send, row_recv, msg_send, msg_recv, out_send, out_recv, mesh_send, mesh_recv, mesh_own):
    patches, ranks = sizes
    me, rank = lax.axis_index("patch"), lax.axis_index("hidden")
    starts, caps, chunks = class_plan(patches)
    far_first = OWN_CHUNKS + 2 * NEAR_CHUNKS
    full = first_w.shape[1]
    width = w_edge.shape[1]
    own_rows = mesh_v.shape[0]
    edge_rows = edge_v.shape[0]
    patch_peer = lambda k: lax.rem(me + k + patches, patches)
    rank_peer = lambda k: lax.rem(rank + k, ranks)
    own_columns = pl.ds(pl.multiple_of(rank * width, width), width)

    def class_of(chunk):
        near = (chunk - OWN_CHUNKS) // NEAR_CHUNKS
        is_near = (chunk >= OWN_CHUNKS) & (chunk < far_first)
        k = jnp.where(chunk < OWN_CHUNKS, 0, jnp.where(is_near, 1 + near * (patches - 2), chunk - far_first + 2))
        at = jnp.where(chunk < OWN_CHUNKS, chunk, jnp.where(is_near, (chunk - OWN_CHUNKS) % NEAR_CHUNKS, 0))
        return k, at

    def send(src, dst, send_sem, recv_sem, axis, peer):
        return pltpu.make_async_remote_copy(
            src_ref=src, dst_ref=dst, send_sem=send_sem, recv_sem=recv_sem,
            device_id={axis: peer}, device_id_type=pl.DeviceIdType.MESH,
        )

    weights = [
        (w_edge, first_w, 0, True),
        (w_sender, first_w, full, True),
        (w_receiver, first_w, 2 * full, True),
        (w_edge_out, second_w, 0, False),
        (w_mesh_in, third_w, 0, True),
        (w_message_in, third_w, full, True),
        (w_mesh_out, fourth_w, 0, False),
    ]

    def landing(entry):
        src, dst, first, by_column = entry
        if by_column:
            return dst.at[pl.ds(first, full), own_columns]
        return dst.at[own_columns, :]

    loads = [
        pltpu.make_async_copy(mesh.at[pl.ds(pl.multiple_of(rank * own_rows, 16), own_rows)], mesh_v, local_sem.at[0]),
        pltpu.make_async_copy(edge, edge_v, local_sem.at[1]),
        pltpu.make_async_copy(grid, grid_v, local_sem.at[2]),
        pltpu.make_async_copy(vector, vectors.at[rank], local_sem.at[3]),
    ]
    for n, entry in enumerate(weights):
        loads.append(pltpu.make_async_copy(entry[0], landing(entry), local_sem.at[4 + n]))
    for load in loads:
        load.start()

    gap = CHUNK - FAR_ROWS
    for chunk in range(far_first, chunks):
        messages[chunk, FAR_ROWS:, :] = jnp.zeros((gap, full), jnp.bfloat16)
    reqs[:CLASS_ROWS, :] = req[:CLASS_ROWS, :]

    barrier = pltpu.get_barrier_semaphore()
    for k in range(1, patches):
        pl.semaphore_signal(barrier, inc=1, device_id={"patch": patch_peer(k)}, device_id_type=pl.DeviceIdType.MESH)
    for k in range(1, ranks):
        pl.semaphore_signal(barrier, inc=1, device_id={"hidden": rank_peer(k)}, device_id_type=pl.DeviceIdType.MESH)
    pl.semaphore_wait(barrier, patches + ranks - 2)

    req_copies = []
    for k in range(1, patches):
        block = pl.ds(k * CLASS_ROWS, CLASS_ROWS)
        copy = send(req.at[block], reqs.at[block], req_send.at[k], req_recv.at[k], "patch", patch_peer(k))
        copy.start()
        req_copies.append(copy)
    weight_copies = []
    for k in range(1, ranks):
        copy = send(vector, vectors.at[rank], weight_send.at[k, 7], weight_recv.at[k, 7], "hidden", rank_peer(k))
        copy.start()
        weight_copies.append(copy)
        for n, entry in enumerate(weights):
            copy = send(entry[0], landing(entry), weight_send.at[k, n], weight_recv.at[k, n], "hidden", rank_peer(k))
            copy.start()
            weight_copies.append(copy)

    def columns(ref, k, at):
        turned = ref[pl.ds(pl.multiple_of(k * CLASS_ROWS, CLASS_ROWS), CLASS_ROWS), :].astype(jnp.float32).T
        lane = iota(turned.shape, 1)
        picks = [jnp.sum(jnp.where(lane == 2 * at + n, turned, 0.0), axis=1, keepdims=True) for n in range(2)]
        return jnp.concatenate(picks, axis=0).astype(jnp.int32)

    def pick(column, source, step):
        total = None
        for first in range(0, source.shape[0], step):
            hot = one_hot(iota((CHUNK, step), 1) == column - first)
            piece = dot(hot, source[first : first + step, :])
            total = piece if total is None else total + piece
        return total.astype(jnp.bfloat16)

    def rows_of(chunk, rows):
        return pl.ds(0, CHUNK if rows is None else rows)

    def row_copy(chunk, k, rows):
        part = pl.ds(0, rows)
        return send(
            rows_out.at[chunk, part], rows_in.at[chunk, part], row_send.at[chunk], row_recv.at[chunk], "patch", patch_peer(-k)
        )

    def msg_copy(chunk, k, rows):
        part = pl.ds(0, rows)
        return send(
            picked_s.at[chunk, part], messages.at[chunk, part], msg_send.at[chunk], msg_recv.at[chunk], "patch", patch_peer(k)
        )

    loads[0].wait()
    gather_step = own_rows if own_rows <= 1280 else CHUNK
    for copy in req_copies:
        copy.wait_recv()

    def serve(chunk, rows):
        k, at = class_of(chunk)
        rows_out[chunk] = pick(columns(reqs, k, at), mesh_v, gather_step)
        row_copy(chunk, k, rows).start()

    @pl.loop(far_first, chunks)
    def _(chunk):
        serve(chunk, FAR_ROWS)

    @pl.loop(OWN_CHUNKS, far_first)
    def _(chunk):
        serve(chunk, CHUNK)

    @pl.loop(0, OWN_CHUNKS)
    def _(chunk):
        rows_in[chunk] = pick(columns(reqs, 0, chunk), mesh_v, gather_step)

    loads[1].wait()
    loads[2].wait()

    @pl.loop(0, chunks)
    def _(chunk):
        k, at = class_of(chunk)
        picked_e[chunk] = pick(columns(edges, k, at), edge_v, 1024)
        picked_s[chunk] = pick(columns(sends, k, at), grid_v, 1024)

    for load in loads[3:]:
        load.wait()
    for copy in weight_copies:
        copy.wait_recv()

    def vector_row(n):
        return jnp.concatenate([vectors[j, n : n + 1, :] for j in range(ranks)], axis=1)

    def edge_mlp(chunk, rows):
        own_edge = picked_e[chunk, :rows, :]
        pre = dot(own_edge, first_w[:full, :])
        pre = pre + dot(picked_s[chunk, :rows, :], first_w[full : 2 * full, :])
        pre = pre + dot(rows_in[chunk, :rows, :], first_w[2 * full :, :]) + vector_row(0)
        hidden = jax.nn.silu(pre).astype(jnp.bfloat16)
        total = dot(hidden, second_w[...]) + vector_row(1)
        message = normalize(total, vector_row(2), vector_row(3))
        result = (own_edge.astype(jnp.float32) + message).astype(jnp.bfloat16)
        for j in range(ranks):
            outgoing[j, chunk, :rows, :] = result[:, j * width : (j + 1) * width]
        return message.astype(jnp.bfloat16)

    @pl.loop(0, OWN_CHUNKS)
    def _(chunk):
        messages[chunk] = edge_mlp(chunk, CHUNK)

    @pl.loop(OWN_CHUNKS, far_first)
    def _(chunk):
        k, _ = class_of(chunk)
        row_copy(chunk, k, CHUNK).wait_recv()
        picked_s[chunk] = edge_mlp(chunk, CHUNK)
        msg_copy(chunk, k, CHUNK).start()

    @pl.loop(far_first, chunks)
    def _(chunk):
        k, _ = class_of(chunk)
        row_copy(chunk, k, FAR_ROWS).wait_recv()
        picked_s[chunk, :FAR_ROWS, :] = edge_mlp(chunk, FAR_ROWS)
        msg_copy(chunk, k, FAR_ROWS).start()

    out_copies = []
    for k in range(1, ranks):
        peer = rank_peer(k)
        spans = [(pl.ds(0, far_first), pl.ds(0, CHUNK)), (pl.ds(far_first, chunks - far_first), pl.ds(0, FAR_ROWS))]
        for n, (block, part) in enumerate(spans):
            copy = send(
                outgoing.at[peer, block, part], incoming.at[rank, block, part],
                out_send.at[k, n], out_recv.at[k, n], "hidden", peer,
            )
            copy.start()
            out_copies.append(copy)

    @pl.loop(OWN_CHUNKS, far_first)
    def _(chunk):
        k, _ = class_of(chunk)
        msg_copy(chunk, k, CHUNK).wait_recv()

    @pl.loop(far_first, chunks)
    def _(chunk):
        k, _ = class_of(chunk)
        msg_copy(chunk, k, FAR_ROWS).wait_recv()

    plan = [(0, c) for c in range(OWN_CHUNKS)] + [(k, c) for k in (1, patches - 1) for c in range(NEAR_CHUNKS)]
    plan += [(k, 0) for k in range(2, patches - 1)]
    blocks = own_rows // CHUNK

    def mesh_copy(block, k):
        peer = rank_peer(k)
        at = pl.ds(pl.multiple_of(rank * own_rows + block * CHUNK, CHUNK), CHUNK)
        return send(
            finished_mesh.at[peer, pl.ds(pl.multiple_of(block * CHUNK, CHUNK), CHUNK)], mesh_out.at[at],
            mesh_send.at[k, block], mesh_recv.at[k, block], "hidden", peer,
        )

    def mesh_local(block):
        at = pl.ds(pl.multiple_of(rank * own_rows + block * CHUNK, CHUNK), CHUNK)
        return pltpu.make_async_copy(
            finished_mesh.at[rank, pl.ds(pl.multiple_of(block * CHUNK, CHUNK), CHUNK)], mesh_out.at[at], mesh_own.at[block]
        )

    @pl.loop(0, blocks)
    def _(block):
        at = pl.ds(pl.multiple_of(block * CHUNK, CHUNK), CHUNK)
        line = iota((CHUNK, CHUNK), 0) + block * CHUNK
        total = None
        for chunk, (k, c) in enumerate(plan):
            row = k * CLASS_ROWS + 2 * c
            wanted = jnp.concatenate([reqs[row : row + 1, :], reqs[row + 1 : row + 2, :]], axis=1)
            piece = dot(one_hot(line == wanted), messages[chunk])
            total = piece if total is None else total + piece
        own = mesh_v[at, :]
        pre = dot(own, third_w[:full, :]) + dot(total.astype(jnp.bfloat16), third_w[full:, :]) + vector_row(4)
        hidden = jax.nn.silu(pre).astype(jnp.bfloat16)
        total = dot(hidden, fourth_w[...]) + vector_row(5)
        update = normalize(total, vector_row(6), vector_row(7))
        result = (own.astype(jnp.float32) + update).astype(jnp.bfloat16)
        for j in range(ranks):
            finished_mesh[j, at, :] = result[:, j * width : (j + 1) * width]
        for k in range(1, ranks):
            mesh_copy(block, k).start()
        mesh_local(block).start()

    over = reqs[CLASS_ROWS - 1 : CLASS_ROWS, :]
    for k in range(1, patches):
        row = (k + 1) * CLASS_ROWS - 1
        over = jnp.maximum(over, reqs[row : row + 1, :])
    flag[...] = jnp.broadcast_to(over, flag.shape)

    for copy in out_copies:
        copy.wait_recv()

    @pl.loop(0, ranks)
    def _(j):
        @pl.when(j == rank)
        def _():
            @pl.loop(0, chunks)
            def _(chunk):
                table[pl.ds(pl.multiple_of((j * chunks + chunk) * CHUNK, CHUNK), CHUNK), :] = outgoing[j, chunk].astype(jnp.float32)

        @pl.when(j != rank)
        def _():
            @pl.loop(0, chunks)
            def _(chunk):
                table[pl.ds(pl.multiple_of((j * chunks + chunk) * CHUNK, CHUNK), CHUNK), :] = incoming[j, chunk].astype(jnp.float32)

    @pl.loop(0, edge_rows // CHUNK)
    def _(block):
        @pl.loop(0, CHUNK // 128)
        def _(line):
            @pl.loop(0, 128, step=16)
            def _(first):
                for n in range(16):
                    spot = where[block * (CHUNK // 128) + line, first + n]
                    staged[pl.ds(line * 128 + first + n, 1), :] = table[pl.ds(spot, 1), :]

        at = pl.ds(pl.multiple_of(block * CHUNK, CHUNK), CHUNK)
        live = iota((CHUNK, width), 0) + block * CHUNK < count[0]
        finished[at, :] = jnp.where(live, staged[...], edge_v[at, own_columns].astype(jnp.float32)).astype(jnp.bfloat16)

    last = pltpu.make_async_copy(finished, edge_out, local_sem.at[0])
    last.start()

    for copy in req_copies + weight_copies + out_copies:
        copy.wait_send()

    @pl.loop(OWN_CHUNKS, far_first)
    def _(chunk):
        k, _ = class_of(chunk)
        row_copy(chunk, k, CHUNK).wait_send()
        msg_copy(chunk, k, CHUNK).wait_send()

    @pl.loop(far_first, chunks)
    def _(chunk):
        k, _ = class_of(chunk)
        row_copy(chunk, k, FAR_ROWS).wait_send()
        msg_copy(chunk, k, FAR_ROWS).wait_send()

    @pl.loop(0, blocks)
    def _(block):
        for k in range(1, ranks):
            mesh_copy(block, k).wait()
        mesh_local(block).wait()

    last.wait()


def run_stages(patches, ranks, count, where, req, edges, sends, vector, weights, mesh_latent, edge_latent, grid_latent):
    full, width = weights[0].shape
    mesh_rows, edge_rows, grid_rows = mesh_latent.shape[0], edge_latent.shape[0], grid_latent.shape[0]
    own_rows = mesh_rows // ranks
    chunks = class_plan(patches)[2]
    bf16, f32 = jnp.bfloat16, jnp.float32
    dma = pltpu.SemaphoreType.DMA
    vmem = pl.BlockSpec(memory_space=pltpu.VMEM)
    smem = pl.BlockSpec(memory_space=pltpu.SMEM)
    hbm = pl.BlockSpec(memory_space=pl.ANY)
    blocks = own_rows // CHUNK
    return pl.pallas_call(
        functools.partial(stage_kernel, (patches, ranks)),
        in_specs=[smem, smem, vmem, vmem, vmem, vmem] + [hbm] * 10,
        out_specs=[hbm, hbm, vmem],
        out_shape=[
            jax.ShapeDtypeStruct((mesh_rows, width), bf16),
            jax.ShapeDtypeStruct((edge_rows, width), bf16),
            jax.ShapeDtypeStruct((8, 128), jnp.int32),
        ],
        scratch_shapes=[
            pltpu.VMEM((own_rows, full), bf16),
            pltpu.VMEM((edge_rows, full), bf16),
            pltpu.VMEM((grid_rows, full), bf16),
            pltpu.VMEM((3 * full, full), bf16),
            pltpu.VMEM((full, full), bf16),
            pltpu.VMEM((2 * full, full), bf16),
            pltpu.VMEM((full, full), bf16),
            pltpu.VMEM((ranks, 8, width), f32),
            pltpu.VMEM((patches * CLASS_ROWS, 128), jnp.int32),
            pltpu.VMEM((chunks, CHUNK, full), bf16),
            pltpu.VMEM((chunks, CHUNK, full), bf16),
            pltpu.VMEM((chunks, CHUNK, full), bf16),
            pltpu.VMEM((chunks, CHUNK, full), bf16),
            pltpu.VMEM((chunks, CHUNK, full), bf16),
            pltpu.VMEM((ranks, chunks, CHUNK, width), bf16),
            pltpu.VMEM((ranks, chunks, CHUNK, width), bf16),
            pltpu.VMEM((ranks * chunks * CHUNK, width), f32),
            pltpu.VMEM((CHUNK, width), f32),
            pltpu.VMEM((edge_rows, width), bf16),
            pltpu.VMEM((ranks, own_rows, width), bf16),
            dma((11,)),
            dma((ranks, 8)),
            dma((ranks, 8)),
            dma((patches,)),
            dma((patches,)),
            dma((chunks,)),
            dma((chunks,)),
            dma((chunks,)),
            dma((chunks,)),
            dma((ranks, 2)),
            dma((ranks, 2)),
            dma((ranks, blocks)),
            dma((ranks, blocks)),
            dma((blocks,)),
        ],
        compiler_params=pltpu.CompilerParams(
            collective_id=0, has_side_effects=True, vmem_limit_bytes=62 * 1024 * 1024
        ),
        name="run_stages",
    )(count, where, req, edges, sends, vector, *weights, mesh_latent, edge_latent, grid_latent)


def pieces(x, axis, size):
    return [x] + [lax.ppermute(x, axis, [((j + k) % size, j) for j in range(size)]) for k in range(1, size)]


def rows_at(x, index):
    return x.at[index].get(mode="promise_in_bounds")


def dense(patches, ranks, operands):
    (grid_latent, mesh_latent, edge_latent, senders, receivers, mesh_slot, edge_counts, w_edge, w_sender, w_receiver,
     edge_bias, w_edge_out, edge_out_bias, edge_gain, edge_shift, w_mesh_in, w_message_in, mesh_bias, w_mesh_out,
     mesh_out_bias, mesh_gain, mesh_shift) = operands
    me, rank = lax.axis_index("patch"), lax.axis_index("hidden")
    mesh_rows, edge_rows = mesh_latent.shape[0], edge_latent.shape[0]
    mesh_total = mesh_slot.shape[0]
    width = w_edge.shape[1]
    bf16 = jnp.bfloat16

    def own(x):
        return lax.dynamic_slice_in_dim(x, rank * width, width, 1)

    def turn(x, axis):
        full = jnp.concatenate(pieces(x, "hidden", ranks), axis)
        return full

    def natural(x):
        full = turn(x, 0)
        return jnp.roll(full, rank * width, 0)[None]

    def spread_mlp(pre, w_out, bias, gain, shift):
        hidden = turn(jax.nn.silu(pre).astype(bf16), 1)
        total = dot(hidden, turn(w_out, 0)) + natural(bias)
        center = jnp.mean(total, axis=1, keepdims=True)
        centered = total - center
        scale = lax.rsqrt(jnp.mean(centered * centered, axis=1, keepdims=True) + EPSILON)
        return own(centered * scale) * gain[None] + shift[None]

    table = jnp.concatenate(pieces(dot(mesh_latent, w_receiver).astype(bf16), "patch", patches), 0)
    target = lax.rem(rows_at(mesh_slot, receivers) + (mesh_total - me * mesh_rows), mesh_total)
    sent = rows_at(dot(grid_latent, w_sender), senders - me * grid_latent.shape[0])
    pre = dot(edge_latent, w_edge) + sent + rows_at(table, target).astype(jnp.float32) + edge_bias[None]
    message = spread_mlp(pre, w_edge_out, edge_out_bias, edge_gain, edge_shift)
    live = jnp.arange(edge_rows)[:, None] < edge_counts[0]
    message = jnp.where(live, message, 0.0)
    edge_out = (own(edge_latent).astype(jnp.float32) + message).astype(bf16)
    sums = jnp.zeros((mesh_total, width), jnp.float32).at[target].add(message, mode="promise_in_bounds")
    summed = sums[:mesh_rows]
    for k in range(1, patches):
        part = sums[k * mesh_rows : (k + 1) * mesh_rows].astype(bf16)
        part = lax.ppermute(part, "patch", [(j, (j + k) % patches) for j in range(patches)])
        summed = summed + part.astype(jnp.float32)
    summed = jnp.roll(turn(summed.astype(bf16), 1), rank * width, 1)
    pre = dot(mesh_latent, w_mesh_in) + dot(summed, w_message_in) + mesh_bias[None]
    update = spread_mlp(pre, w_mesh_out, mesh_out_bias, mesh_gain, mesh_shift)
    mesh_out = (own(mesh_latent).astype(jnp.float32) + update).astype(bf16)
    return mesh_out, edge_out


def shards(patches, ranks, *operands):
    (grid_latent, mesh_latent, edge_latent, senders, receivers, mesh_slot, edge_counts, w_edge, w_sender, w_receiver,
     edge_bias, w_edge_out, edge_out_bias, edge_gain, edge_shift, w_mesh_in, w_message_in, mesh_bias, w_mesh_out,
     mesh_out_bias, mesh_gain, mesh_shift) = operands
    mesh_rows, edge_rows, grid_rows = mesh_latent.shape[0], edge_latent.shape[0], grid_latent.shape[0]
    fits = (
        w_edge.shape[1] % 128 == 0
        and 4 < patches <= 16
        and edge_rows % 1024 == 0
        and grid_rows % 1024 == 0
        and mesh_rows % (ranks * CHUNK) == 0
        and mesh_slot.shape[0] % 1024 == 0
    )
    if not fits:
        return dense(patches, ranks, operands)
    me = lax.axis_index("patch").astype(jnp.int32)
    rank = lax.axis_index("hidden").astype(jnp.int32)
    here = jnp.stack([me, rank, edge_counts[0]])
    req, edges, sends, where = plan_edges(
        here, receivers, senders - me * grid_rows, mesh_slot, patches, ranks, mesh_rows
    )
    vector = jnp.stack(
        [edge_bias, edge_out_bias, edge_gain, edge_shift, mesh_bias, mesh_out_bias, mesh_gain, mesh_shift]
    )
    weights = (w_edge, w_sender, w_receiver, w_edge_out, w_mesh_in, w_message_in, w_mesh_out)
    mesh_out, edge_out, flag = run_stages(
        patches, ranks, edge_counts, where, req, edges, sends, vector, weights, mesh_latent, edge_latent, grid_latent
    )
    return lax.cond(
        flag[0, 0] > 0,
        lambda outs, args: dense(patches, ranks, args),
        lambda outs, args: outs,
        (mesh_out, edge_out),
        operands,
    )


def solution(mesh):
    columns, rows, line, patch = P(None, "hidden"), P("hidden", None), P("hidden"), P("patch", None)
    return jax.shard_map(
        functools.partial(shards, mesh.shape["patch"], mesh.shape["hidden"]),
        mesh=mesh,
        in_specs=(
            patch, patch, patch, P("patch"), P("patch"), P(), P("patch"),
            columns, columns, columns, line, rows, line, line, line,
            columns, columns, line, rows, line, line, line,
        ),
        out_specs=(P("patch", "hidden"), P("patch", "hidden")),
        check_vma=False,
    )
```

```python
import functools

import jax
import jax.numpy as jnp
from jax import lax
from jax.experimental import pallas as pl
from jax.experimental.pallas import tpu as pltpu
from jax.sharding import PartitionSpec as P

EPSILON = 1e-05
CHUNK = 256
OWN_CHUNKS = 3
NEAR_CHUNKS = 2
NEAR_ROWS = 240
FAR_ROWS = 176
CLASS_ROWS = 8


def iota(shape, axis):
    return lax.broadcasted_iota(jnp.int32, shape, axis)


def one_hot(cond):
    return jnp.where(cond, 1.0, 0.0).astype(jnp.bfloat16)


def dot(a, b):
    return jnp.dot(a, b, preferred_element_type=jnp.float32)


def dot_nt(a, b):
    return lax.dot_general(a, b, (((1,), (1,)), ((), ())), preferred_element_type=jnp.float32)


def within(index, size):
    if size & (size - 1) == 0:
        return index & (size - 1)
    return jnp.clip(index, 0, size - 1)


def wide(block):
    return jnp.concatenate([block[j : j + 1, :] for j in range(block.shape[0])], axis=1)


def normalize(total, gain, offset):
    width = total.shape[1]
    center = jnp.sum(total, axis=1, keepdims=True) / width
    centered = total - center
    spread = jnp.sum(centered * centered, axis=1, keepdims=True) / width
    return centered * lax.rsqrt(spread + EPSILON) * gain + offset


def class_plan(patches):
    starts = [0, OWN_CHUNKS] + [OWN_CHUNKS + 2 * NEAR_CHUNKS + k - 2 for k in range(2, patches - 1)]
    starts.append(OWN_CHUNKS + NEAR_CHUNKS)
    near = NEAR_CHUNKS * NEAR_ROWS
    caps = [OWN_CHUNKS * CHUNK, near] + [FAR_ROWS] * (patches - 3) + [near]
    return starts, caps, OWN_CHUNKS + 2 * NEAR_CHUNKS + patches - 3


def plan_edges(sizes, me, rank_me, count, recv_ref, send_ref, slot_ref, req_ref, edge_ref, send_out_ref, where_ref, slots, target, masks, position, local, totals):
    patches, ranks, mesh_rows, grid_rows, parts = sizes
    groups = recv_ref.shape[0]
    own_rows = mesh_rows // ranks
    starts, caps, chunks = class_plan(patches)
    high = slot_ref.shape[0]
    turned = slot_ref[...].astype(jnp.float32).T.astype(jnp.int32)
    for part in range(parts):
        slots[part * 128 : (part + 1) * 128, :] = ((turned >> (8 * part)) & 255).astype(jnp.float32).astype(jnp.bfloat16)

    def lookup(i, carry):
        row = wide(recv_ref[pl.ds(i * 8, 8), :])
        hot = one_hot(iota((high, 1024), 0) == (row >> 7))
        found = dot(slots[...], hot)
        low = iota((128, 1024), 0) == (row & 127)
        value = jnp.zeros((1, 1024), jnp.float32)
        for part in range(parts):
            piece = jnp.where(low, found[part * 128 : (part + 1) * 128], 0.0)
            value = value + float(256**part) * jnp.sum(piece, axis=0, keepdims=True)
        value = value.astype(jnp.int32)
        block = jnp.concatenate([value[:, j * 128 : (j + 1) * 128] for j in range(8)], axis=0)
        target[pl.ds(i * 8, 8), :] = block
        return carry

    lax.fori_loop(0, groups // 8, lookup, 0)

    shape = (groups, 128)
    goal = target[...]
    owner = sum((goal >= k * mesh_rows).astype(jnp.int32) for k in range(1, patches))
    inside = goal - owner * mesh_rows
    part = sum((inside >= k * own_rows).astype(jnp.int32) for k in range(1, ranks))
    offset = owner - me
    offset = jnp.where(offset < 0, offset + patches, offset)
    slot = iota(shape, 0) * 128 + iota(shape, 1)
    live = slot < count
    label = jnp.where(live, offset * ranks + part, -1)
    classes = patches * ranks
    for c in range(classes):
        masks[c * groups : (c + 1) * groups, :] = one_hot(label == c)
    steps = jnp.concatenate([one_hot(iota((128, 128), 0) <= iota((128, 128), 1)), jnp.ones((128, 128), jnp.bfloat16)], axis=1)
    totals[...] = dot(masks[...], steps)
    below = one_hot(iota((groups, groups), 1) < iota((groups, groups), 0))
    rank = jnp.zeros(shape, jnp.float32)
    over = jnp.zeros((1, 128), jnp.float32)
    for c in range(classes):
        block = totals[c * groups : (c + 1) * groups, :]
        inner, whole = block[:, :128], block[:, 128:]
        before = dot(below, whole.astype(jnp.bfloat16))
        mine = jnp.where(label == c, 1.0, 0.0)
        rank = rank + mine * (inner - 1.0 + before)
        full = before[groups - 1 :, :] + whole[groups - 1 :, :]
        over = jnp.maximum(over, jnp.where(full > float(caps[c // ranks]), 1.0, 0.0))
    rank = rank.astype(jnp.int32)
    first = jnp.zeros(shape, jnp.int32)
    cap = jnp.zeros(shape, jnp.int32)
    for k in range(patches):
        first = jnp.where(offset == k, starts[k] * CHUNK, first)
        cap = jnp.where(offset == k, caps[k], cap)
    fits = rank < cap
    near = (offset == 1) | (offset == patches - 1)
    rank = jnp.where(near & (rank >= NEAR_ROWS), rank + (CHUNK - NEAR_ROWS), rank)
    spot = part * (chunks * CHUNK) + first + rank
    spot = jnp.clip(spot, 0, ranks * chunks * CHUNK - 1)
    where_ref[...] = jnp.where(live, spot, 0)
    mine = live & (part == rank_me) & fits
    position[...] = jnp.where(mine, offset * (CLASS_ROWS * 128) + rank, -1)
    local[...] = inside - rank_me * own_rows

    rows = patches * CLASS_ROWS

    def invert(i, total):
        at = pl.ds(i * 8, 8)
        spots = wide(position[at, :])
        edge = i * 1024 + iota((1, 1024), 1)
        line = wide(local[at, :])
        sender = wide(send_ref[at, :]) - me * grid_rows
        here = iota((rows, 1024), 0) == (spots >> 7)
        values = [jnp.ones((1, 1024), jnp.int32)]
        for value in (line, edge, sender):
            values += [value >> 8, value & 255]
        left = jnp.concatenate(
            [jnp.where(here, value.astype(jnp.float32), 0.0).astype(jnp.bfloat16) for value in values], axis=0
        )
        right = one_hot(iota((128, 1024), 0) == (spots & 127))
        return total + dot_nt(left, right)

    total = lax.fori_loop(0, groups // 8, invert, jnp.zeros((7 * rows, 128), jnp.float32))
    filled = total[:rows] > 0.5

    def value_of(n, empty):
        value = total[n * rows : (n + 1) * rows] * 256.0 + total[(n + 1) * rows : (n + 2) * rows]
        return jnp.where(filled, value, empty).astype(jnp.int32)

    last = (iota((rows, 128), 0) & (CLASS_ROWS - 1)) == CLASS_ROWS - 1
    req_ref[...] = jnp.where(last, over.astype(jnp.int32), value_of(1, -1.0))
    edge_ref[...] = jnp.clip(value_of(3, 0.0), 0, groups * 128 - 1)
    send_out_ref[...] = value_of(5, 0.0)


def stage_kernel(sizes, count, receivers, senders, mesh_slot, bias_a, bias_b, gain_a, shift_a, bias_c, bias_d, gain_b, shift_b, w_edge, w_sender, w_receiver, w_edge_out, w_mesh_in, w_message_in, w_mesh_out, mesh, edge, grid, mesh_out, edge_out, flag, mesh_v, edge_v, grid_v, first_w, second_w, third_w, fourth_w, vectors, req, reqs, edges, sends, places, slots, target, masks, position, local, totals, edge_s, where, rows_out, rows_in, results, messages, outgoing, incoming, table, gathered, staged, finished, finished_mesh, local_sem, weight_send, weight_recv, req_send, req_recv, row_send, row_recv, msg_send, msg_recv, out_send, out_recv, mesh_send, mesh_recv, mesh_own):
    patches, ranks = sizes[0], sizes[1]
    me, rank = lax.axis_index("patch"), lax.axis_index("hidden")
    chunks = class_plan(patches)[2]
    far_first = OWN_CHUNKS + 2 * NEAR_CHUNKS
    full = first_w.shape[1]
    width = w_edge.shape[1]
    own_rows = mesh_v.shape[0]
    edge_rows = edge_v.shape[0]
    patch_peer = lambda k: lax.rem(me + k + patches, patches)
    rank_peer = lambda k: lax.rem(rank + k, ranks)
    side = rank + 1 - 2 * lax.rem(rank, 2)
    across = lax.rem(rank + 2, ranks)

    def class_of(chunk):
        near = (chunk - OWN_CHUNKS) // NEAR_CHUNKS
        is_near = (chunk >= OWN_CHUNKS) & (chunk < far_first)
        k = jnp.where(chunk < OWN_CHUNKS, 0, jnp.where(is_near, 1 + near * (patches - 2), chunk - far_first + 2))
        at = jnp.where(chunk < OWN_CHUNKS, chunk, jnp.where(is_near, (chunk - OWN_CHUNKS) % NEAR_CHUNKS, 0))
        return k, at

    def send(src, dst, send_sem, recv_sem, axis, peer):
        return pltpu.make_async_remote_copy(
            src_ref=src, dst_ref=dst, send_sem=send_sem, recv_sem=recv_sem,
            device_id={axis: peer}, device_id_type=pl.DeviceIdType.MESH,
        )

    weights = [
        (w_edge, first_w, 0, True),
        (w_sender, first_w, full, True),
        (w_receiver, first_w, 2 * full, True),
        (w_edge_out, second_w, 0, False),
        (w_mesh_in, third_w, 0, True),
        (w_message_in, third_w, full, True),
        (w_mesh_out, fourth_w, 0, False),
    ]
    edge_weights, mesh_weights = [7, 0, 1, 2, 3], [4, 5, 6]

    def landing(n, owner):
        if n == 7:
            return vectors.at[owner]
        _, dst, first, by_column = weights[n]
        columns = pl.ds(pl.multiple_of(owner * width, width), width)
        if by_column:
            return dst.at[pl.ds(first, full), columns]
        return dst.at[columns, :]

    def weight_copy(n, way):
        source = landing(n, across) if way == 2 else (vectors.at[rank] if n == 7 else weights[n][0])
        owner = across if way == 2 else rank
        peer = across if way == 1 else side
        return send(source, landing(n, owner), weight_send.at[way, n], weight_recv.at[way, n], "hidden", peer)

    loads = [
        pltpu.make_async_copy(mesh.at[pl.ds(pl.multiple_of(rank * own_rows, 16), own_rows)], mesh_v, local_sem.at[0]),
        pltpu.make_async_copy(edge, edge_v, local_sem.at[1]),
        pltpu.make_async_copy(grid, grid_v, local_sem.at[2]),
    ]
    for n, entry in enumerate(weights):
        loads.append(pltpu.make_async_copy(entry[0], landing(n, rank), local_sem.at[3 + n]))
    for load in loads:
        load.start()

    barrier = pltpu.get_barrier_semaphore()
    for k in range(1, patches):
        pl.semaphore_signal(barrier, inc=1, device_id={"patch": patch_peer(k)}, device_id_type=pl.DeviceIdType.MESH)
    for k in range(1, ranks):
        pl.semaphore_signal(barrier, inc=1, device_id={"hidden": rank_peer(k)}, device_id_type=pl.DeviceIdType.MESH)

    vectors[rank] = jnp.concatenate(
        [ref[...] for ref in (bias_a, bias_b, gain_a, shift_a, bias_c, bias_d, gain_b, shift_b)], axis=0
    )
    for chunk in range(OWN_CHUNKS, far_first):
        messages[chunk, NEAR_ROWS:, :] = jnp.zeros((CHUNK - NEAR_ROWS, full), jnp.bfloat16)
    for chunk in range(far_first, chunks):
        messages[chunk, FAR_ROWS:, :] = jnp.zeros((CHUNK - FAR_ROWS, full), jnp.bfloat16)

    pl.semaphore_wait(barrier, patches + ranks - 2)
    for n in edge_weights + mesh_weights:
        weight_copy(n, 1).start()
        weight_copy(n, 0).start()

    plan_edges(sizes, me, rank, count[0], receivers, senders, mesh_slot, req, edges, sends, places, slots, target, masks, position, local, totals)

    req_copies = []
    for k in range(1, patches):
        block = pl.ds(k * CLASS_ROWS, CLASS_ROWS)
        copy = send(req.at[block], reqs.at[block], req_send.at[k], req_recv.at[k], "patch", patch_peer(k))
        copy.start()
        req_copies.append(copy)
    reqs[:CLASS_ROWS, :] = req[:CLASS_ROWS, :]
    scalars = [
        pltpu.make_async_copy(edges, edge_s, local_sem.at[10]),
        pltpu.make_async_copy(places, where, local_sem.at[11]),
    ]
    for copy in scalars:
        copy.start()

    loads[1].wait()

    @pl.loop(0, edge_rows // CHUNK)
    def _(block):
        at = pl.multiple_of(block * CHUNK, CHUNK)
        for j in range(ranks):
            table[pl.ds(j * edge_rows + at, CHUNK), :] = edge_v[pl.ds(at, CHUNK), j * width : (j + 1) * width].astype(jnp.float32)

    def columns(ref, k, at):
        turned = ref[pl.ds(pl.multiple_of(k * CLASS_ROWS, CLASS_ROWS), CLASS_ROWS), :].astype(jnp.float32).T
        lane = iota(turned.shape, 1)
        picks = [jnp.sum(jnp.where(lane == 2 * at + n, turned, 0.0), axis=1, keepdims=True) for n in range(2)]
        return jnp.concatenate(picks, axis=0).astype(jnp.int32)

    def pick(column, source, step):
        total = None
        for first in range(0, source.shape[0], step):
            hot = one_hot(iota((column.shape[0], step), 1) == column - first)
            piece = dot(hot, source[first : first + step, :])
            total = piece if total is None else total + piece
        return total.astype(jnp.bfloat16)

    def row_copy(chunk, k, rows):
        part = pl.ds(0, rows)
        return send(
            rows_out.at[chunk, part], rows_in.at[chunk, part], row_send.at[chunk], row_recv.at[chunk], "patch", patch_peer(-k)
        )

    def msg_copy(chunk, k, rows):
        part = pl.ds(0, rows)
        return send(
            results.at[chunk, part], messages.at[chunk, part], msg_send.at[chunk], msg_recv.at[chunk], "patch", patch_peer(k)
        )

    def out_copy(chunk, k, rows):
        peer, part = rank_peer(k), pl.ds(0, rows)
        return send(
            outgoing.at[peer, chunk, part], incoming.at[rank, chunk, part],
            out_send.at[k, chunk], out_recv.at[k, chunk], "hidden", peer,
        )

    loads[0].wait()
    gather_step = own_rows if own_rows <= 1280 else CHUNK
    for copy in req_copies:
        copy.wait_recv()

    def serve(chunk, rows):
        k, at = class_of(chunk)
        rows_out[chunk] = pick(columns(reqs, k, at), mesh_v, gather_step)
        row_copy(chunk, k, rows).start()

    @pl.loop(far_first, chunks)
    def _(chunk):
        serve(chunk, FAR_ROWS)

    @pl.loop(OWN_CHUNKS, far_first)
    def _(chunk):
        serve(chunk, NEAR_ROWS)

    loads[2].wait()
    for copy in scalars:
        copy.wait()
    for load in loads[3:]:
        load.wait()
    for n in edge_weights:
        weight_copy(n, 1).wait_recv()
        weight_copy(n, 2).start()

    @pl.loop(0, OWN_CHUNKS)
    def _(chunk):
        rows_in[chunk] = pick(columns(reqs, 0, chunk), mesh_v, gather_step)

    for n in edge_weights:
        weight_copy(n, 0).wait_recv()
        weight_copy(n, 2).wait_recv()

    def vector_row(n):
        return jnp.concatenate([vectors[j, n : n + 1, :] for j in range(ranks)], axis=1)

    def collect(line, first, amount):
        for n in range(amount):
            spot = within(edge_s[line, n], edge_rows)
            for j in range(ranks):
                gathered[first + n : first + n + 1, j * width : (j + 1) * width] = table[pl.ds(j * edge_rows + spot, 1), :]

    def edge_stage(chunk, rows):
        k, at = class_of(chunk)
        collect(k * CLASS_ROWS + 2 * at, 0, 128)
        collect(k * CLASS_ROWS + 2 * at + 1, 128, rows - 128)
        own_edge = gathered[:rows, :]
        pre = dot(own_edge.astype(jnp.bfloat16), first_w[:full, :])
        sender = pick(columns(sends, k, at)[:rows], grid_v, 1024)
        pre = pre + dot(sender, first_w[full : 2 * full, :])
        return own_edge, pre

    def edge_finish(chunk, rows, own_edge, pre):
        pre = pre + dot(rows_in[chunk, :rows, :], first_w[2 * full :, :]) + vector_row(0)
        hidden = jax.nn.silu(pre).astype(jnp.bfloat16)
        total = dot(hidden, second_w[...]) + vector_row(1)
        message = normalize(total, vector_row(2), vector_row(3))
        result = (own_edge + message).astype(jnp.bfloat16)
        for j in range(ranks):
            outgoing[j, chunk, :rows, :] = result[:, j * width : (j + 1) * width]
        return message.astype(jnp.bfloat16)

    def remote_chunk(chunk, rows):
        k, _ = class_of(chunk)
        own_edge, pre = edge_stage(chunk, rows)
        row_copy(chunk, k, rows).wait_recv()
        results[chunk, :rows, :] = edge_finish(chunk, rows, own_edge, pre)
        msg_copy(chunk, k, rows).start()
        for j in range(1, ranks):
            out_copy(chunk, j, rows).start()

    @pl.loop(far_first, chunks)
    def _(chunk):
        remote_chunk(chunk, FAR_ROWS)

    @pl.loop(OWN_CHUNKS, far_first)
    def _(chunk):
        remote_chunk(chunk, NEAR_ROWS)

    @pl.loop(0, OWN_CHUNKS)
    def _(chunk):
        own_edge, pre = edge_stage(chunk, CHUNK)
        messages[chunk] = edge_finish(chunk, CHUNK, own_edge, pre)
        for j in range(1, ranks):
            out_copy(chunk, j, CHUNK).start()

    for n in mesh_weights:
        weight_copy(n, 1).wait_recv()
        weight_copy(n, 2).start()

    def each_chunk(act):
        @pl.loop(0, OWN_CHUNKS)
        def _(chunk):
            act(chunk, CHUNK, False)

        @pl.loop(OWN_CHUNKS, far_first)
        def _(chunk):
            act(chunk, NEAR_ROWS, True)

        @pl.loop(far_first, chunks)
        def _(chunk):
            act(chunk, FAR_ROWS, True)

    def await_out(chunk, rows, remote):
        for j in range(1, ranks):
            out_copy(chunk, j, rows).wait_recv()

    each_chunk(await_out)

    @pl.loop(0, ranks)
    def _(j):
        @pl.when(j == rank)
        def _():
            @pl.loop(0, chunks)
            def _(chunk):
                table[pl.ds(pl.multiple_of((j * chunks + chunk) * CHUNK, CHUNK), CHUNK), :] = outgoing[j, chunk].astype(jnp.float32)

        @pl.when(j != rank)
        def _():
            @pl.loop(0, chunks)
            def _(chunk):
                table[pl.ds(pl.multiple_of((j * chunks + chunk) * CHUNK, CHUNK), CHUNK), :] = incoming[j, chunk].astype(jnp.float32)

    own_columns = pl.ds(pl.multiple_of(rank * width, width), width)

    @pl.loop(0, edge_rows // 128)
    def _(line):
        for n in range(128):
            spot = within(where[line, n], table.shape[0])
            staged[n : n + 1, :] = table[pl.ds(spot, 1), :]
        at = pl.ds(pl.multiple_of(line * 128, 128), 128)
        live = iota((128, width), 0) + line * 128 < count[0]
        finished[at, :] = jnp.where(live, staged[...], edge_v[at, own_columns].astype(jnp.float32)).astype(jnp.bfloat16)

    last = pltpu.make_async_copy(finished, edge_out, local_sem.at[0])
    last.start()

    for n in mesh_weights:
        weight_copy(n, 0).wait_recv()
        weight_copy(n, 2).wait_recv()

    def await_msg(chunk, rows, remote):
        if remote:
            msg_copy(chunk, class_of(chunk)[0], rows).wait_recv()

    each_chunk(await_msg)

    plan = [(0, c) for c in range(OWN_CHUNKS)] + [(k, c) for k in (1, patches - 1) for c in range(NEAR_CHUNKS)]
    plan += [(k, 0) for k in range(2, patches - 1)]
    blocks = own_rows // CHUNK

    def mesh_copy(block, k):
        peer = rank_peer(k)
        at = pl.ds(pl.multiple_of(rank * own_rows + block * CHUNK, CHUNK), CHUNK)
        return send(
            finished_mesh.at[peer, pl.ds(pl.multiple_of(block * CHUNK, CHUNK), CHUNK)], mesh_out.at[at],
            mesh_send.at[k, block], mesh_recv.at[k, block], "hidden", peer,
        )

    def mesh_local(block):
        at = pl.ds(pl.multiple_of(rank * own_rows + block * CHUNK, CHUNK), CHUNK)
        return pltpu.make_async_copy(
            finished_mesh.at[rank, pl.ds(pl.multiple_of(block * CHUNK, CHUNK), CHUNK)], mesh_out.at[at], mesh_own.at[block]
        )

    @pl.loop(0, blocks)
    def _(block):
        at = pl.ds(pl.multiple_of(block * CHUNK, CHUNK), CHUNK)
        line = iota((CHUNK, CHUNK), 0) + block * CHUNK
        total = None
        for chunk, (k, c) in enumerate(plan):
            row = k * CLASS_ROWS + 2 * c
            wanted = jnp.concatenate([reqs[row : row + 1, :], reqs[row + 1 : row + 2, :]], axis=1)
            piece = dot(one_hot(line == wanted), messages[chunk])
            total = piece if total is None else total + piece
        own = mesh_v[at, :]
        pre = dot(own, third_w[:full, :]) + dot(total.astype(jnp.bfloat16), third_w[full:, :]) + vector_row(4)
        hidden = jax.nn.silu(pre).astype(jnp.bfloat16)
        total = dot(hidden, fourth_w[...]) + vector_row(5)
        update = normalize(total, vector_row(6), vector_row(7))
        result = (own.astype(jnp.float32) + update).astype(jnp.bfloat16)
        for j in range(ranks):
            finished_mesh[j, at, :] = result[:, j * width : (j + 1) * width]
        for k in range(1, ranks):
            mesh_copy(block, k).start()
        mesh_local(block).start()

    over = reqs[CLASS_ROWS - 1 : CLASS_ROWS, :]
    for k in range(1, patches):
        row = (k + 1) * CLASS_ROWS - 1
        over = jnp.maximum(over, reqs[row : row + 1, :])
    flag[...] = jnp.broadcast_to(over, flag.shape)

    for copy in req_copies:
        copy.wait_send()
    for way in range(3):
        for n in edge_weights + mesh_weights:
            weight_copy(n, way).wait_send()

    def drain(chunk, rows, remote):
        for j in range(1, ranks):
            out_copy(chunk, j, rows).wait_send()
        if remote:
            k = class_of(chunk)[0]
            row_copy(chunk, k, rows).wait_send()
            msg_copy(chunk, k, rows).wait_send()

    each_chunk(drain)

    @pl.loop(0, blocks)
    def _(block):
        for k in range(1, ranks):
            mesh_copy(block, k).wait()
        mesh_local(block).wait()

    last.wait()


def run_stages(patches, ranks, count, receivers, senders, mesh_slot, vectors, weights, mesh_latent, edge_latent, grid_latent):
    full, width = weights[0].shape
    mesh_rows, edge_rows, grid_rows = mesh_latent.shape[0], edge_latent.shape[0], grid_latent.shape[0]
    own_rows = mesh_rows // ranks
    chunks = class_plan(patches)[2]
    groups, high = edge_rows // 128, mesh_slot.shape[0] // 128
    parts = 1
    while 256**parts < mesh_slot.shape[0]:
        parts += 1
    bf16, f32, i32 = jnp.bfloat16, jnp.float32, jnp.int32
    dma = pltpu.SemaphoreType.DMA
    vmem = pl.BlockSpec(memory_space=pltpu.VMEM)
    smem = pl.BlockSpec(memory_space=pltpu.SMEM)
    hbm = pl.BlockSpec(memory_space=pl.ANY)
    blocks = own_rows // CHUNK
    lists = patches * CLASS_ROWS
    classes = patches * ranks * groups
    return pl.pallas_call(
        functools.partial(stage_kernel, (patches, ranks, mesh_rows, grid_rows, parts)),
        in_specs=[smem] + [vmem] * 11 + [hbm] * 10,
        out_specs=[hbm, hbm, vmem],
        out_shape=[
            jax.ShapeDtypeStruct((mesh_rows, width), bf16),
            jax.ShapeDtypeStruct((edge_rows, width), bf16),
            jax.ShapeDtypeStruct((8, 128), i32),
        ],
        scratch_shapes=[
            pltpu.VMEM((own_rows, full), bf16),
            pltpu.VMEM((edge_rows, full), bf16),
            pltpu.VMEM((grid_rows, full), bf16),
            pltpu.VMEM((3 * full, full), bf16),
            pltpu.VMEM((full, full), bf16),
            pltpu.VMEM((2 * full, full), bf16),
            pltpu.VMEM((full, full), bf16),
            pltpu.VMEM((ranks, 8, width), f32),
            pltpu.VMEM((lists, 128), i32),
            pltpu.VMEM((lists, 128), i32),
            pltpu.VMEM((lists, 128), i32),
            pltpu.VMEM((lists, 128), i32),
            pltpu.VMEM((groups, 128), i32),
            pltpu.VMEM((parts * 128, high), bf16),
            pltpu.VMEM((groups, 128), i32),
            pltpu.VMEM((classes, 128), bf16),
            pltpu.VMEM((groups, 128), i32),
            pltpu.VMEM((groups, 128), i32),
            pltpu.VMEM((classes, 256), f32),
            pltpu.SMEM((lists, 128), i32),
            pltpu.SMEM((groups, 128), i32),
            pltpu.VMEM((chunks, CHUNK, full), bf16),
            pltpu.VMEM((chunks, CHUNK, full), bf16),
            pltpu.VMEM((chunks, CHUNK, full), bf16),
            pltpu.VMEM((chunks, CHUNK, full), bf16),
            pltpu.VMEM((ranks, chunks, CHUNK, width), bf16),
            pltpu.VMEM((ranks, chunks, CHUNK, width), bf16),
            pltpu.VMEM((ranks * max(edge_rows, chunks * CHUNK), width), f32),
            pltpu.VMEM((CHUNK, full), f32),
            pltpu.VMEM((128, width), f32),
            pltpu.VMEM((edge_rows, width), bf16),
            pltpu.VMEM((ranks, own_rows, width), bf16),
            dma((12,)),
            dma((3, 8)),
            dma((3, 8)),
            dma((patches,)),
            dma((patches,)),
            dma((chunks,)),
            dma((chunks,)),
            dma((chunks,)),
            dma((chunks,)),
            dma((ranks, chunks)),
            dma((ranks, chunks)),
            dma((ranks, blocks)),
            dma((ranks, blocks)),
            dma((blocks,)),
        ],
        compiler_params=pltpu.CompilerParams(
            collective_id=0, has_side_effects=True, vmem_limit_bytes=67043328
        ),
        name="run_stages",
    )(
        count, receivers.reshape(groups, 128), senders.reshape(groups, 128), mesh_slot.reshape(high, 128),
        *[vector[None] for vector in vectors], *weights, mesh_latent, edge_latent, grid_latent,
    )


def pieces(x, axis, size):
    return [x] + [lax.ppermute(x, axis, [((j + k) % size, j) for j in range(size)]) for k in range(1, size)]


def rows_at(x, index):
    return x.at[index].get(mode="promise_in_bounds")


def dense(patches, ranks, operands):
    (grid_latent, mesh_latent, edge_latent, senders, receivers, mesh_slot, edge_counts, w_edge, w_sender, w_receiver,
     edge_bias, w_edge_out, edge_out_bias, edge_gain, edge_shift, w_mesh_in, w_message_in, mesh_bias, w_mesh_out,
     mesh_out_bias, mesh_gain, mesh_shift) = operands
    me, rank = lax.axis_index("patch"), lax.axis_index("hidden")
    mesh_rows, edge_rows = mesh_latent.shape[0], edge_latent.shape[0]
    mesh_total = mesh_slot.shape[0]
    width = w_edge.shape[1]
    bf16 = jnp.bfloat16

    def own(x):
        return lax.dynamic_slice_in_dim(x, rank * width, width, 1)

    def turn(x, axis):
        full = jnp.concatenate(pieces(x, "hidden", ranks), axis)
        return full

    def natural(x):
        full = turn(x, 0)
        return jnp.roll(full, rank * width, 0)[None]

    def spread_mlp(pre, w_out, bias, gain, shift):
        w_full, bias_full = turn(w_out, 0), natural(bias)
        step = CHUNK if pre.shape[0] % CHUNK == 0 else pre.shape[0]

        def block(i, result):
            part = lax.dynamic_slice_in_dim(pre, i * step, step, 0)
            hidden = turn(jax.nn.silu(part).astype(bf16), 1)
            total = dot(hidden, w_full) + bias_full
            center = jnp.mean(total, axis=1, keepdims=True)
            centered = total - center
            scale = lax.rsqrt(jnp.mean(centered * centered, axis=1, keepdims=True) + EPSILON)
            update = own(centered * scale) * gain[None] + shift[None]
            return lax.dynamic_update_slice_in_dim(result, update, i * step, 0)

        return lax.fori_loop(0, pre.shape[0] // step, block, jnp.zeros(pre.shape, jnp.float32))

    table = jnp.concatenate(pieces(dot(mesh_latent, w_receiver).astype(bf16), "patch", patches), 0)
    target = lax.rem(rows_at(mesh_slot, receivers) + (mesh_total - me * mesh_rows), mesh_total)
    sent = rows_at(dot(grid_latent, w_sender), senders - me * grid_latent.shape[0])
    pre = dot(edge_latent, w_edge) + sent + rows_at(table, target).astype(jnp.float32) + edge_bias[None]
    message = spread_mlp(pre, w_edge_out, edge_out_bias, edge_gain, edge_shift)
    live = jnp.arange(edge_rows)[:, None] < edge_counts[0]
    message = jnp.where(live, message, 0.0)
    edge_out = (own(edge_latent).astype(jnp.float32) + message).astype(bf16)
    rounded = message.astype(bf16)

    def add_block(i, sums):
        hot = (target[None] == (i * CHUNK + jnp.arange(CHUNK))[:, None]).astype(bf16)
        return lax.dynamic_update_slice_in_dim(sums, dot(hot, rounded), i * CHUNK, 0)

    sums = jnp.zeros((mesh_total, width), jnp.float32)
    if mesh_total % CHUNK:
        sums = sums.at[target].add(message, mode="promise_in_bounds")
    else:
        sums = lax.fori_loop(0, mesh_total // CHUNK, add_block, sums)
    summed = sums[:mesh_rows]
    for k in range(1, patches):
        part = sums[k * mesh_rows : (k + 1) * mesh_rows].astype(bf16)
        part = lax.ppermute(part, "patch", [(j, (j + k) % patches) for j in range(patches)])
        summed = summed + part.astype(jnp.float32)
    summed = jnp.roll(turn(summed.astype(bf16), 1), rank * width, 1)
    pre = dot(mesh_latent, w_mesh_in) + dot(summed, w_message_in) + mesh_bias[None]
    update = spread_mlp(pre, w_mesh_out, mesh_out_bias, mesh_gain, mesh_shift)
    mesh_out = (own(mesh_latent).astype(jnp.float32) + update).astype(bf16)
    return mesh_out, edge_out


def shards(patches, ranks, *operands):
    (grid_latent, mesh_latent, edge_latent, senders, receivers, mesh_slot, edge_counts, w_edge, w_sender, w_receiver,
     edge_bias, w_edge_out, edge_out_bias, edge_gain, edge_shift, w_mesh_in, w_message_in, mesh_bias, w_mesh_out,
     mesh_out_bias, mesh_gain, mesh_shift) = operands
    mesh_rows, edge_rows, grid_rows = mesh_latent.shape[0], edge_latent.shape[0], grid_latent.shape[0]
    fits = (
        w_edge.shape[1] % 128 == 0
        and ranks == 4
        and 4 < patches <= 16
        and edge_rows % 1024 == 0
        and grid_rows % 1024 == 0
        and mesh_rows % (ranks * CHUNK) == 0
        and mesh_slot.shape[0] % 1024 == 0
    )
    if not fits:
        return dense(patches, ranks, operands)
    vectors = (edge_bias, edge_out_bias, edge_gain, edge_shift, mesh_bias, mesh_out_bias, mesh_gain, mesh_shift)
    weights = (w_edge, w_sender, w_receiver, w_edge_out, w_mesh_in, w_message_in, w_mesh_out)
    mesh_out, edge_out, flag = run_stages(
        patches, ranks, edge_counts, receivers, senders, mesh_slot, vectors, weights, mesh_latent, edge_latent, grid_latent
    )
    return lax.cond(
        flag[0, 0] > 0,
        lambda outs, args: dense(patches, ranks, args),
        lambda outs, args: outs,
        (mesh_out, edge_out),
        operands,
    )


def solution(mesh):
    columns, rows, line, patch = P(None, "hidden"), P("hidden", None), P("hidden"), P("patch", None)
    return jax.shard_map(
        functools.partial(shards, mesh.shape["patch"], mesh.shape["hidden"]),
        mesh=mesh,
        in_specs=(
            patch, patch, patch, P("patch"), P("patch"), P(), P("patch"),
            columns, columns, columns, line, rows, line, line, line,
            columns, columns, line, rows, line, line, line,
        ),
        out_specs=(P("patch", "hidden"), P("patch", "hidden")),
        check_vma=False,
    )
```

```python
import functools

import jax
import jax.numpy as jnp
from jax import lax
from jax.experimental import pallas as pl
from jax.experimental.pallas import tpu as pltpu
from jax.sharding import PartitionSpec as P

EPSILON = 1e-05
CHUNK = 256
OWN_CHUNKS = 3
NEAR_CHUNKS = 2
NEAR_ROWS = 240
FAR_ROWS = 176
CLASS_ROWS = 8


def iota(shape, axis):
    return lax.broadcasted_iota(jnp.int32, shape, axis)


def one_hot(cond):
    return jnp.where(cond, 1.0, 0.0).astype(jnp.bfloat16)


def dot(a, b):
    return jnp.dot(a, b, preferred_element_type=jnp.float32)


def dot_nt(a, b):
    return lax.dot_general(a, b, (((1,), (1,)), ((), ())), preferred_element_type=jnp.float32)


def within(index, size):
    if size & (size - 1) == 0:
        return index & (size - 1)
    return jnp.clip(index, 0, size - 1)


def wide(block):
    return jnp.concatenate([block[j : j + 1, :] for j in range(block.shape[0])], axis=1)


def normalize(total, gain, offset):
    width = total.shape[1]
    center = jnp.sum(total, axis=1, keepdims=True) / width
    centered = total - center
    spread = jnp.sum(centered * centered, axis=1, keepdims=True) / width
    return centered * lax.rsqrt(spread + EPSILON) * gain + offset


def class_plan(patches):
    starts = [0, OWN_CHUNKS] + [OWN_CHUNKS + 2 * NEAR_CHUNKS + k - 2 for k in range(2, patches - 1)]
    starts.append(OWN_CHUNKS + NEAR_CHUNKS)
    near = NEAR_CHUNKS * NEAR_ROWS
    caps = [OWN_CHUNKS * CHUNK, near] + [FAR_ROWS] * (patches - 3) + [near]
    return starts, caps, OWN_CHUNKS + 2 * NEAR_CHUNKS + patches - 3


def plan_edges(sizes, me, rank_me, count, recv_ref, send_ref, slot_ref, req_ref, edge_ref, send_out_ref, where_ref, slots, target, masks, position, local, totals):
    patches, ranks, mesh_rows, grid_rows, parts = sizes
    groups = recv_ref.shape[0]
    own_rows = mesh_rows // ranks
    starts, caps, chunks = class_plan(patches)
    high = slot_ref.shape[0]
    turned = slot_ref[...].astype(jnp.float32).T.astype(jnp.int32)
    for part in range(parts):
        slots[part * 128 : (part + 1) * 128, :] = ((turned >> (8 * part)) & 255).astype(jnp.float32).astype(jnp.bfloat16)

    def lookup(i, carry):
        row = wide(recv_ref[pl.ds(i * 8, 8), :])
        hot = one_hot(iota((high, 1024), 0) == (row >> 7))
        found = dot(slots[...], hot)
        low = iota((128, 1024), 0) == (row & 127)
        value = jnp.zeros((1, 1024), jnp.float32)
        for part in range(parts):
            piece = jnp.where(low, found[part * 128 : (part + 1) * 128], 0.0)
            value = value + float(256**part) * jnp.sum(piece, axis=0, keepdims=True)
        value = value.astype(jnp.int32)
        block = jnp.concatenate([value[:, j * 128 : (j + 1) * 128] for j in range(8)], axis=0)
        target[pl.ds(i * 8, 8), :] = block
        return carry

    lax.fori_loop(0, groups // 8, lookup, 0, unroll=2)

    shape = (groups, 128)
    goal = target[...]
    owner = sum((goal >= k * mesh_rows).astype(jnp.int32) for k in range(1, patches))
    inside = goal - owner * mesh_rows
    part = sum((inside >= k * own_rows).astype(jnp.int32) for k in range(1, ranks))
    offset = owner - me
    offset = jnp.where(offset < 0, offset + patches, offset)
    slot = iota(shape, 0) * 128 + iota(shape, 1)
    live = slot < count
    label = jnp.where(live, offset * ranks + part, -1)
    classes = patches * ranks
    for c in range(classes):
        masks[c * groups : (c + 1) * groups, :] = one_hot(label == c)
    steps = jnp.concatenate([one_hot(iota((128, 128), 0) <= iota((128, 128), 1)), jnp.ones((128, 128), jnp.bfloat16)], axis=1)
    totals[...] = dot(masks[...], steps)
    below = one_hot(iota((groups, groups), 1) < iota((groups, groups), 0))
    rank = jnp.zeros(shape, jnp.float32)
    over = jnp.zeros((1, 128), jnp.float32)
    for c in range(classes):
        block = totals[c * groups : (c + 1) * groups, :]
        inner, whole = block[:, :128], block[:, 128:]
        before = dot(below, whole.astype(jnp.bfloat16))
        mine = jnp.where(label == c, 1.0, 0.0)
        rank = rank + mine * (inner - 1.0 + before)
        full = before[groups - 1 :, :] + whole[groups - 1 :, :]
        over = jnp.maximum(over, jnp.where(full > float(caps[c // ranks]), 1.0, 0.0))
    rank = rank.astype(jnp.int32)
    first = jnp.zeros(shape, jnp.int32)
    cap = jnp.zeros(shape, jnp.int32)
    for k in range(patches):
        first = jnp.where(offset == k, starts[k] * CHUNK, first)
        cap = jnp.where(offset == k, caps[k], cap)
    fits = rank < cap
    near = (offset == 1) | (offset == patches - 1)
    rank = jnp.where(near & (rank >= NEAR_ROWS), rank + (CHUNK - NEAR_ROWS), rank)
    spot = part * (chunks * CHUNK) + first + rank
    spot = jnp.clip(spot, 0, ranks * chunks * CHUNK - 1)
    where_ref[...] = jnp.where(live, spot, 0)
    mine = live & (part == rank_me) & fits
    position[...] = jnp.where(mine, offset * (CLASS_ROWS * 128) + rank, -1)
    local[...] = inside - rank_me * own_rows

    rows = patches * CLASS_ROWS

    def invert(read, amount):
        def step(i, total):
            at = pl.ds(i * 8, 8)
            spots = wide(position[at, :])
            here = iota((rows, 1024), 0) == (spots >> 7)
            values = [part for value in read(i, at) for part in (value >> 8, value & 255)]
            left = jnp.concatenate(
                [jnp.where(here, value.astype(jnp.float32), 0.0).astype(jnp.bfloat16) for value in values], axis=0
            )
            right = one_hot(iota((128, 1024), 0) == (spots & 127))
            return total + dot_nt(left, right)

        total = lax.fori_loop(0, groups // 8, step, jnp.zeros((2 * amount * rows, 128), jnp.float32))
        pairs = [total[n * rows : (n + 1) * rows] for n in range(2 * amount)]
        return [(pairs[2 * n] * 256.0 + pairs[2 * n + 1]).astype(jnp.int32) for n in range(amount)]

    last = (iota((rows, 128), 0) & (CLASS_ROWS - 1)) == CLASS_ROWS - 1
    asked = invert(lambda i, at: [wide(local[at, :]) + 1], 1)[0] - 1
    req_ref[...] = jnp.where(last, over.astype(jnp.int32), asked)

    def finish():
        edge, sender = invert(
            lambda i, at: [i * 1024 + iota((1, 1024), 1), wide(send_ref[at, :]) - me * grid_rows], 2
        )
        edge_ref[...] = jnp.clip(edge, 0, groups * 128 - 1)
        send_out_ref[...] = sender

    return finish


def stage_kernel(sizes, count, receivers, senders, mesh_slot, bias_a, bias_b, gain_a, shift_a, bias_c, bias_d, gain_b, shift_b, w_edge, w_sender, w_receiver, w_edge_out, w_mesh_in, w_message_in, w_mesh_out, mesh, edge, grid, mesh_out, edge_out, flag, mesh_v, edge_v, grid_v, first_w, second_w, third_w, fourth_w, vectors, req, reqs, edges, sends, places, slots, target, masks, position, local, totals, edge_s, where, rows_out, rows_in, results, messages, outgoing, incoming, table, gathered, staged, finished, finished_mesh, summed, local_sem, weight_send, weight_recv, req_send, req_recv, row_send, row_recv, msg_send, msg_recv, out_send, out_recv, mesh_send, mesh_recv, mesh_own):
    patches, ranks = sizes[0], sizes[1]
    me, rank = lax.axis_index("patch"), lax.axis_index("hidden")
    chunks = class_plan(patches)[2]
    far_first = OWN_CHUNKS + 2 * NEAR_CHUNKS
    full = first_w.shape[1]
    width = w_edge.shape[1]
    own_rows = mesh_v.shape[0]
    edge_rows = edge_v.shape[0]
    patch_peer = lambda k: lax.rem(me + k + patches, patches)
    rank_peer = lambda k: lax.rem(rank + k, ranks)
    side = rank + 1 - 2 * lax.rem(rank, 2)
    across = lax.rem(rank + 2, ranks)

    def class_of(chunk):
        near = (chunk - OWN_CHUNKS) // NEAR_CHUNKS
        is_near = (chunk >= OWN_CHUNKS) & (chunk < far_first)
        k = jnp.where(chunk < OWN_CHUNKS, 0, jnp.where(is_near, 1 + near * (patches - 2), chunk - far_first + 2))
        at = jnp.where(chunk < OWN_CHUNKS, chunk, jnp.where(is_near, (chunk - OWN_CHUNKS) % NEAR_CHUNKS, 0))
        return k, at

    def send(src, dst, send_sem, recv_sem, axis, peer):
        return pltpu.make_async_remote_copy(
            src_ref=src, dst_ref=dst, send_sem=send_sem, recv_sem=recv_sem,
            device_id={axis: peer}, device_id_type=pl.DeviceIdType.MESH,
        )

    weights = [
        (w_edge, first_w, 0, True),
        (w_sender, first_w, full, True),
        (w_receiver, first_w, 2 * full, True),
        (w_edge_out, second_w, 0, False),
        (w_mesh_in, third_w, 0, True),
        (w_message_in, third_w, full, True),
        (w_mesh_out, fourth_w, 0, False),
    ]
    edge_weights, mesh_weights = [7, 0, 1, 2, 3], [4, 5, 6]

    def landing(n, owner):
        if n == 7:
            return vectors.at[owner]
        _, dst, first, by_column = weights[n]
        columns = pl.ds(pl.multiple_of(owner * width, width), width)
        if by_column:
            return dst.at[pl.ds(first, full), columns]
        return dst.at[columns, :]

    def weight_copy(n, way):
        source = landing(n, across) if way == 2 else (vectors.at[rank] if n == 7 else weights[n][0])
        owner = across if way == 2 else rank
        peer = across if way == 1 else side
        return send(source, landing(n, owner), weight_send.at[way, n], weight_recv.at[way, n], "hidden", peer)

    loads = [
        pltpu.make_async_copy(mesh.at[pl.ds(pl.multiple_of(rank * own_rows, 16), own_rows)], mesh_v, local_sem.at[0]),
        pltpu.make_async_copy(edge, edge_v, local_sem.at[1]),
        pltpu.make_async_copy(grid, grid_v, local_sem.at[2]),
    ]
    for n, entry in enumerate(weights):
        loads.append(pltpu.make_async_copy(entry[0], landing(n, rank), local_sem.at[3 + n]))
    for load in loads:
        load.start()

    barrier = pltpu.get_barrier_semaphore()
    for k in range(1, patches):
        pl.semaphore_signal(barrier, inc=1, device_id={"patch": patch_peer(k)}, device_id_type=pl.DeviceIdType.MESH)
    for k in range(1, ranks):
        pl.semaphore_signal(barrier, inc=1, device_id={"hidden": rank_peer(k)}, device_id_type=pl.DeviceIdType.MESH)

    vectors[rank] = jnp.concatenate(
        [ref[...] for ref in (bias_a, bias_b, gain_a, shift_a, bias_c, bias_d, gain_b, shift_b)], axis=0
    )
    for chunk in range(OWN_CHUNKS, far_first):
        messages[chunk, NEAR_ROWS:, :] = jnp.zeros((CHUNK - NEAR_ROWS, full), jnp.bfloat16)
    for chunk in range(far_first, chunks):
        messages[chunk, FAR_ROWS:, :] = jnp.zeros((CHUNK - FAR_ROWS, full), jnp.bfloat16)

    pl.semaphore_wait(barrier, patches + ranks - 2)
    for n in edge_weights + mesh_weights:
        weight_copy(n, 1).start()
        weight_copy(n, 0).start()

    finish_plan = plan_edges(sizes, me, rank, count[0], receivers, senders, mesh_slot, req, edges, sends, places, slots, target, masks, position, local, totals)

    req_copies = []
    for k in range(1, patches):
        block = pl.ds(k * CLASS_ROWS, CLASS_ROWS)
        copy = send(req.at[block], reqs.at[block], req_send.at[k], req_recv.at[k], "patch", patch_peer(k))
        copy.start()
        req_copies.append(copy)
    reqs[:CLASS_ROWS, :] = req[:CLASS_ROWS, :]
    finish_plan()
    scalars = [
        pltpu.make_async_copy(edges, edge_s, local_sem.at[10]),
        pltpu.make_async_copy(places, where, local_sem.at[11]),
    ]
    for copy in scalars:
        copy.start()

    loads[1].wait()

    @pl.loop(0, edge_rows // CHUNK)
    def _(block):
        at = pl.multiple_of(block * CHUNK, CHUNK)
        for j in range(ranks):
            table[pl.ds(j * edge_rows + at, CHUNK), :] = edge_v[pl.ds(at, CHUNK), j * width : (j + 1) * width].astype(jnp.float32)

    def columns(ref, k, at):
        turned = ref[pl.ds(pl.multiple_of(k * CLASS_ROWS, CLASS_ROWS), CLASS_ROWS), :].astype(jnp.float32).T
        lane = iota(turned.shape, 1)
        picks = [jnp.sum(jnp.where(lane == 2 * at + n, turned, 0.0), axis=1, keepdims=True) for n in range(2)]
        return jnp.concatenate(picks, axis=0).astype(jnp.int32)

    def pick(column, source, step):
        total = None
        for first in range(0, source.shape[0], step):
            hot = one_hot(iota((column.shape[0], step), 1) == column - first)
            piece = dot(hot, source[first : first + step, :])
            total = piece if total is None else total + piece
        return total.astype(jnp.bfloat16)

    def row_copy(chunk, k, rows):
        part = pl.ds(0, rows)
        return send(
            rows_out.at[chunk, part], rows_in.at[chunk, part], row_send.at[chunk], row_recv.at[chunk], "patch", patch_peer(-k)
        )

    def msg_copy(chunk, k, rows):
        part = pl.ds(0, rows)
        return send(
            results.at[chunk, part], messages.at[chunk, part], msg_send.at[chunk], msg_recv.at[chunk], "patch", patch_peer(k)
        )

    def out_copy(chunk, k, rows):
        peer, part = rank_peer(k), pl.ds(0, rows)
        return send(
            outgoing.at[peer, chunk, part], incoming.at[rank, chunk, part],
            out_send.at[k, chunk], out_recv.at[k, chunk], "hidden", peer,
        )

    loads[0].wait()
    gather_step = own_rows if own_rows <= 1280 else CHUNK
    for copy in req_copies:
        copy.wait_recv()

    def serve(chunk, rows):
        k, at = class_of(chunk)
        rows_out[chunk, :rows, :] = pick(columns(reqs, k, at)[:rows], mesh_v, gather_step)
        row_copy(chunk, k, rows).start()

    far_count, near_count = chunks - far_first, far_first - OWN_CHUNKS

    def in_turn(act):
        @pl.loop(0, max(far_count, near_count))
        def _(j):
            @pl.when(j < far_count)
            def _():
                act(far_first + j, FAR_ROWS)

            @pl.when(j < near_count)
            def _():
                act(OWN_CHUNKS + j, NEAR_ROWS)

    in_turn(serve)

    loads[2].wait()
    for copy in scalars:
        copy.wait()
    for load in loads[3:]:
        load.wait()
    for n in edge_weights:
        weight_copy(n, 1).wait_recv()
        weight_copy(n, 2).start()

    @pl.loop(0, OWN_CHUNKS)
    def _(chunk):
        rows_in[chunk] = pick(columns(reqs, 0, chunk), mesh_v, gather_step)

    for n in edge_weights:
        weight_copy(n, 0).wait_recv()
        weight_copy(n, 2).wait_recv()

    def vector_row(n):
        return jnp.concatenate([vectors[j, n : n + 1, :] for j in range(ranks)], axis=1)

    def collect(line, first, amount):
        for n in range(amount):
            spot = within(edge_s[line, n], edge_rows)
            for j in range(ranks):
                gathered[j, pl.ds(first + n, 1), :] = table[pl.ds(j * edge_rows + spot, 1), :]

    def edge_stage(chunk, rows):
        k, at = class_of(chunk)
        if rows == CHUNK:
            @pl.loop(0, 2)
            def _(half):
                collect(k * CLASS_ROWS + 2 * at + half, pl.multiple_of(half * 128, 128), 128)
        else:
            collect(k * CLASS_ROWS + 2 * at, 0, 128)
            collect(k * CLASS_ROWS + 2 * at + 1, 128, rows - 128)
        own_edge = jnp.concatenate([gathered[j, :rows, :] for j in range(ranks)], axis=1)
        pre = dot(own_edge.astype(jnp.bfloat16), first_w[:full, :])
        sender = pick(columns(sends, k, at)[:rows], grid_v, 1024)
        pre = pre + dot(sender, first_w[full : 2 * full, :])
        return own_edge, pre

    def edge_finish(chunk, rows, own_edge, pre):
        pre = pre + dot(rows_in[chunk, :rows, :], first_w[2 * full :, :]) + vector_row(0)
        hidden = jax.nn.silu(pre).astype(jnp.bfloat16)
        total = dot(hidden, second_w[...]) + vector_row(1)
        message = normalize(total, vector_row(2), vector_row(3))
        result = (own_edge + message).astype(jnp.bfloat16)
        for j in range(ranks):
            outgoing[j, chunk, :rows, :] = result[:, j * width : (j + 1) * width]
        return message.astype(jnp.bfloat16)

    def remote_chunk(chunk, rows):
        k, _ = class_of(chunk)
        own_edge, pre = edge_stage(chunk, rows)
        row_copy(chunk, k, rows).wait_recv()
        results[chunk, :rows, :] = edge_finish(chunk, rows, own_edge, pre)
        msg_copy(chunk, k, rows).start()
        for j in range(1, ranks):
            out_copy(chunk, j, rows).start()

    @pl.loop(0, OWN_CHUNKS)
    def _(chunk):
        own_edge, pre = edge_stage(chunk, CHUNK)
        messages[chunk] = edge_finish(chunk, CHUNK, own_edge, pre)
        for j in range(1, ranks):
            out_copy(chunk, j, CHUNK).start()

    in_turn(remote_chunk)

    for n in mesh_weights:
        weight_copy(n, 1).wait_recv()
        weight_copy(n, 2).start()

    def each_chunk(act):
        @pl.loop(0, OWN_CHUNKS)
        def _(chunk):
            act(chunk, CHUNK, False)

        @pl.loop(OWN_CHUNKS, far_first)
        def _(chunk):
            act(chunk, NEAR_ROWS, True)

        @pl.loop(far_first, chunks)
        def _(chunk):
            act(chunk, FAR_ROWS, True)

    def await_out(chunk, rows, remote):
        for j in range(1, ranks):
            out_copy(chunk, j, rows).wait_recv()

    blocks = own_rows // CHUNK

    def await_message(chunk, rows):
        msg_copy(chunk, class_of(chunk)[0], rows).wait_recv()

    def add_messages(chunk):
        k, at = class_of(chunk)
        row = pl.multiple_of(k * CLASS_ROWS, CLASS_ROWS)
        asked = reqs[pl.ds(row, CLASS_ROWS), :]
        line = iota(asked.shape, 0)
        pair = [jnp.sum(jnp.where(line == 2 * at + n, asked, 0), axis=0, keepdims=True) for n in range(2)]
        wanted = jnp.concatenate(pair, axis=1)
        for block in range(blocks):
            span = slice(block * CHUNK, (block + 1) * CHUNK)
            hot = one_hot(iota((CHUNK, CHUNK), 0) + block * CHUNK == wanted)
            summed[span, :] += dot(hot, messages[chunk])

    summed[...] = jnp.zeros(summed.shape, jnp.float32)

    @pl.loop(0, OWN_CHUNKS)
    def _(chunk):
        add_messages(chunk)

    each_chunk(await_out)

    @pl.loop(0, ranks)
    def _(j):
        @pl.when(j == rank)
        def _():
            @pl.loop(0, chunks)
            def _(chunk):
                table[pl.ds(pl.multiple_of((j * chunks + chunk) * CHUNK, CHUNK), CHUNK), :] = outgoing[j, chunk].astype(jnp.float32)

        @pl.when(j != rank)
        def _():
            @pl.loop(0, chunks)
            def _(chunk):
                table[pl.ds(pl.multiple_of((j * chunks + chunk) * CHUNK, CHUNK), CHUNK), :] = incoming[j, chunk].astype(jnp.float32)

    own_columns = pl.ds(pl.multiple_of(rank * width, width), width)

    @pl.loop(0, edge_rows // 128)
    def _(line):
        for n in range(128):
            spot = within(where[line, n], table.shape[0])
            staged[n : n + 1, :] = table[pl.ds(spot, 1), :]
        at = pl.ds(pl.multiple_of(line * 128, 128), 128)
        live = iota((128, width), 0) + line * 128 < count[0]
        finished[at, :] = jnp.where(live, staged[...], edge_v[at, own_columns].astype(jnp.float32)).astype(jnp.bfloat16)

    last = pltpu.make_async_copy(finished, edge_out, local_sem.at[0])
    last.start()

    for n in mesh_weights:
        weight_copy(n, 0).wait_recv()
        weight_copy(n, 2).wait_recv()

    def mesh_copy(block, k):
        peer = rank_peer(k)
        at = pl.ds(pl.multiple_of(rank * own_rows + block * CHUNK, CHUNK), CHUNK)
        return send(
            finished_mesh.at[peer, pl.ds(pl.multiple_of(block * CHUNK, CHUNK), CHUNK)], mesh_out.at[at],
            mesh_send.at[k, block], mesh_recv.at[k, block], "hidden", peer,
        )

    def mesh_local(block):
        at = pl.ds(pl.multiple_of(rank * own_rows + block * CHUNK, CHUNK), CHUNK)
        return pltpu.make_async_copy(
            finished_mesh.at[rank, pl.ds(pl.multiple_of(block * CHUNK, CHUNK), CHUNK)], mesh_out.at[at], mesh_own.at[block]
        )

    @pl.loop(0, far_count + near_count)
    def _(j):
        paired = 2 * min(far_count, near_count)
        odd = lax.rem(j, 2)
        rest = (far_first if far_count > near_count else OWN_CHUNKS) + j - paired // 2
        chunk = jnp.where(j < paired, jnp.where(odd == 0, far_first, OWN_CHUNKS) + j // 2, rest)

        @pl.when(chunk >= far_first)
        def _():
            await_message(chunk, FAR_ROWS)

        @pl.when(chunk < far_first)
        def _():
            await_message(chunk, NEAR_ROWS)

        add_messages(chunk)

    @pl.loop(0, blocks)
    def _(block):
        at = pl.ds(pl.multiple_of(block * CHUNK, CHUNK), CHUNK)
        own = mesh_v[at, :]
        pre = dot(own, third_w[:full, :]) + dot(summed[at, :].astype(jnp.bfloat16), third_w[full:, :]) + vector_row(4)
        hidden = jax.nn.silu(pre).astype(jnp.bfloat16)
        total = dot(hidden, fourth_w[...]) + vector_row(5)
        update = normalize(total, vector_row(6), vector_row(7))
        result = (own.astype(jnp.float32) + update).astype(jnp.bfloat16)
        for j in range(ranks):
            finished_mesh[j, at, :] = result[:, j * width : (j + 1) * width]
        for k in range(1, ranks):
            mesh_copy(block, k).start()
        mesh_local(block).start()

    over = reqs[CLASS_ROWS - 1 : CLASS_ROWS, :]
    for k in range(1, patches):
        row = (k + 1) * CLASS_ROWS - 1
        over = jnp.maximum(over, reqs[row : row + 1, :])
    flag[...] = jnp.broadcast_to(over, flag.shape)

    for copy in req_copies:
        copy.wait_send()
    for way in range(3):
        for n in edge_weights + mesh_weights:
            weight_copy(n, way).wait_send()

    def drain(chunk, rows, remote):
        for j in range(1, ranks):
            out_copy(chunk, j, rows).wait_send()
        if remote:
            k = class_of(chunk)[0]
            row_copy(chunk, k, rows).wait_send()
            msg_copy(chunk, k, rows).wait_send()

    each_chunk(drain)

    @pl.loop(0, blocks)
    def _(block):
        for k in range(1, ranks):
            mesh_copy(block, k).wait()
        mesh_local(block).wait()

    last.wait()


def run_stages(patches, ranks, count, receivers, senders, mesh_slot, vectors, weights, mesh_latent, edge_latent, grid_latent):
    full, width = weights[0].shape
    mesh_rows, edge_rows, grid_rows = mesh_latent.shape[0], edge_latent.shape[0], grid_latent.shape[0]
    own_rows = mesh_rows // ranks
    chunks = class_plan(patches)[2]
    groups, high = edge_rows // 128, mesh_slot.shape[0] // 128
    parts = 1
    while 256**parts < mesh_slot.shape[0]:
        parts += 1
    bf16, f32, i32 = jnp.bfloat16, jnp.float32, jnp.int32
    dma = pltpu.SemaphoreType.DMA
    vmem = pl.BlockSpec(memory_space=pltpu.VMEM)
    smem = pl.BlockSpec(memory_space=pltpu.SMEM)
    hbm = pl.BlockSpec(memory_space=pl.ANY)
    blocks = own_rows // CHUNK
    lists = patches * CLASS_ROWS
    classes = patches * ranks * groups
    return pl.pallas_call(
        functools.partial(stage_kernel, (patches, ranks, mesh_rows, grid_rows, parts)),
        in_specs=[smem] + [vmem] * 11 + [hbm] * 10,
        out_specs=[hbm, hbm, vmem],
        out_shape=[
            jax.ShapeDtypeStruct((mesh_rows, width), bf16),
            jax.ShapeDtypeStruct((edge_rows, width), bf16),
            jax.ShapeDtypeStruct((8, 128), i32),
        ],
        scratch_shapes=[
            pltpu.VMEM((own_rows, full), bf16),
            pltpu.VMEM((edge_rows, full), bf16),
            pltpu.VMEM((grid_rows, full), bf16),
            pltpu.VMEM((3 * full, full), bf16),
            pltpu.VMEM((full, full), bf16),
            pltpu.VMEM((2 * full, full), bf16),
            pltpu.VMEM((full, full), bf16),
            pltpu.VMEM((ranks, 8, width), f32),
            pltpu.VMEM((lists, 128), i32),
            pltpu.VMEM((lists, 128), i32),
            pltpu.VMEM((lists, 128), i32),
            pltpu.VMEM((lists, 128), i32),
            pltpu.VMEM((groups, 128), i32),
            pltpu.VMEM((parts * 128, high), bf16),
            pltpu.VMEM((groups, 128), i32),
            pltpu.VMEM((classes, 128), bf16),
            pltpu.VMEM((groups, 128), i32),
            pltpu.VMEM((groups, 128), i32),
            pltpu.VMEM((classes, 256), f32),
            pltpu.SMEM((lists, 128), i32),
            pltpu.SMEM((groups, 128), i32),
            pltpu.VMEM((chunks, CHUNK, full), bf16),
            pltpu.VMEM((chunks, CHUNK, full), bf16),
            pltpu.VMEM((chunks, CHUNK, full), bf16),
            pltpu.VMEM((chunks, CHUNK, full), bf16),
            pltpu.VMEM((ranks, chunks, CHUNK, width), bf16),
            pltpu.VMEM((ranks, chunks, CHUNK, width), bf16),
            pltpu.VMEM((ranks * max(edge_rows, chunks * CHUNK), width), f32),
            pltpu.VMEM((ranks, CHUNK, width), f32),
            pltpu.VMEM((128, width), f32),
            pltpu.VMEM((edge_rows, width), bf16),
            pltpu.VMEM((ranks, own_rows, width), bf16),
            pltpu.VMEM((own_rows, full), f32),
            dma((12,)),
            dma((3, 8)),
            dma((3, 8)),
            dma((patches,)),
            dma((patches,)),
            dma((chunks,)),
            dma((chunks,)),
            dma((chunks,)),
            dma((chunks,)),
            dma((ranks, chunks)),
            dma((ranks, chunks)),
            dma((ranks, blocks)),
            dma((ranks, blocks)),
            dma((blocks,)),
        ],
        compiler_params=pltpu.CompilerParams(
            collective_id=0, has_side_effects=True, vmem_limit_bytes=67043328
        ),
        name="run_stages",
    )(
        count, receivers.reshape(groups, 128), senders.reshape(groups, 128), mesh_slot.reshape(high, 128),
        *[vector[None] for vector in vectors], *weights, mesh_latent, edge_latent, grid_latent,
    )


def pieces(x, axis, size):
    return [x] + [lax.ppermute(x, axis, [((j + k) % size, j) for j in range(size)]) for k in range(1, size)]


def rows_at(x, index):
    return x.at[index].get(mode="promise_in_bounds")


def dense(patches, ranks, operands):
    (grid_latent, mesh_latent, edge_latent, senders, receivers, mesh_slot, edge_counts, w_edge, w_sender, w_receiver,
     edge_bias, w_edge_out, edge_out_bias, edge_gain, edge_shift, w_mesh_in, w_message_in, mesh_bias, w_mesh_out,
     mesh_out_bias, mesh_gain, mesh_shift) = operands
    me, rank = lax.axis_index("patch"), lax.axis_index("hidden")
    mesh_rows, edge_rows = mesh_latent.shape[0], edge_latent.shape[0]
    mesh_total = mesh_slot.shape[0]
    width = w_edge.shape[1]
    bf16 = jnp.bfloat16

    def own(x):
        return lax.dynamic_slice_in_dim(x, rank * width, width, 1)

    def turn(x, axis):
        full = jnp.concatenate(pieces(x, "hidden", ranks), axis)
        return full

    def natural(x):
        full = turn(x, 0)
        return jnp.roll(full, rank * width, 0)[None]

    def spread_mlp(pre, w_out, bias, gain, shift):
        w_full, bias_full = turn(w_out, 0), natural(bias)
        step = CHUNK if pre.shape[0] % CHUNK == 0 else pre.shape[0]

        def block(i, result):
            part = lax.dynamic_slice_in_dim(pre, i * step, step, 0)
            hidden = turn(jax.nn.silu(part).astype(bf16), 1)
            total = dot(hidden, w_full) + bias_full
            center = jnp.mean(total, axis=1, keepdims=True)
            centered = total - center
            scale = lax.rsqrt(jnp.mean(centered * centered, axis=1, keepdims=True) + EPSILON)
            update = own(centered * scale) * gain[None] + shift[None]
            return lax.dynamic_update_slice_in_dim(result, update, i * step, 0)

        return lax.fori_loop(0, pre.shape[0] // step, block, jnp.zeros(pre.shape, jnp.float32))

    table = jnp.concatenate(pieces(dot(mesh_latent, w_receiver).astype(bf16), "patch", patches), 0)
    target = lax.rem(rows_at(mesh_slot, receivers) + (mesh_total - me * mesh_rows), mesh_total)
    sent = rows_at(dot(grid_latent, w_sender), senders - me * grid_latent.shape[0])
    pre = dot(edge_latent, w_edge) + sent + rows_at(table, target).astype(jnp.float32) + edge_bias[None]
    message = spread_mlp(pre, w_edge_out, edge_out_bias, edge_gain, edge_shift)
    live = jnp.arange(edge_rows)[:, None] < edge_counts[0]
    message = jnp.where(live, message, 0.0)
    edge_out = (own(edge_latent).astype(jnp.float32) + message).astype(bf16)
    rounded = message.astype(bf16)

    def add_block(i, sums):
        hot = (target[None] == (i * CHUNK + jnp.arange(CHUNK))[:, None]).astype(bf16)
        return lax.dynamic_update_slice_in_dim(sums, dot(hot, rounded), i * CHUNK, 0)

    sums = jnp.zeros((mesh_total, width), jnp.float32)
    if mesh_total % CHUNK:
        sums = sums.at[target].add(message, mode="promise_in_bounds")
    else:
        sums = lax.fori_loop(0, mesh_total // CHUNK, add_block, sums)
    summed = sums[:mesh_rows]
    for k in range(1, patches):
        part = sums[k * mesh_rows : (k + 1) * mesh_rows].astype(bf16)
        part = lax.ppermute(part, "patch", [(j, (j + k) % patches) for j in range(patches)])
        summed = summed + part.astype(jnp.float32)
    summed = jnp.roll(turn(summed.astype(bf16), 1), rank * width, 1)
    pre = dot(mesh_latent, w_mesh_in) + dot(summed, w_message_in) + mesh_bias[None]
    update = spread_mlp(pre, w_mesh_out, mesh_out_bias, mesh_gain, mesh_shift)
    mesh_out = (own(mesh_latent).astype(jnp.float32) + update).astype(bf16)
    return mesh_out, edge_out


def shards(patches, ranks, *operands):
    (grid_latent, mesh_latent, edge_latent, senders, receivers, mesh_slot, edge_counts, w_edge, w_sender, w_receiver,
     edge_bias, w_edge_out, edge_out_bias, edge_gain, edge_shift, w_mesh_in, w_message_in, mesh_bias, w_mesh_out,
     mesh_out_bias, mesh_gain, mesh_shift) = operands
    mesh_rows, edge_rows, grid_rows = mesh_latent.shape[0], edge_latent.shape[0], grid_latent.shape[0]
    fits = (
        w_edge.shape[1] % 128 == 0
        and ranks == 4
        and 4 < patches <= 16
        and edge_rows % 1024 == 0
        and grid_rows % 1024 == 0
        and mesh_rows % (ranks * CHUNK) == 0
        and mesh_slot.shape[0] % 1024 == 0
    )
    if not fits:
        return dense(patches, ranks, operands)
    vectors = (edge_bias, edge_out_bias, edge_gain, edge_shift, mesh_bias, mesh_out_bias, mesh_gain, mesh_shift)
    weights = (w_edge, w_sender, w_receiver, w_edge_out, w_mesh_in, w_message_in, w_mesh_out)
    mesh_out, edge_out, flag = run_stages(
        patches, ranks, edge_counts, receivers, senders, mesh_slot, vectors, weights, mesh_latent, edge_latent, grid_latent
    )
    return lax.cond(
        flag[0, 0] > 0,
        lambda outs, args: dense(patches, ranks, args),
        lambda outs, args: outs,
        (mesh_out, edge_out),
        operands,
    )


def solution(mesh):
    columns, rows, line, patch = P(None, "hidden"), P("hidden", None), P("hidden"), P("patch", None)
    return jax.shard_map(
        functools.partial(shards, mesh.shape["patch"], mesh.shape["hidden"]),
        mesh=mesh,
        in_specs=(
            patch, patch, patch, P("patch"), P("patch"), P(), P("patch"),
            columns, columns, columns, line, rows, line, line, line,
            columns, columns, line, rows, line, line, line,
        ),
        out_specs=(P("patch", "hidden"), P("patch", "hidden")),
        check_vma=False,
    )
```

```python
import functools

import jax
import jax.numpy as jnp
from jax import lax
from jax.experimental import pallas as pl
from jax.experimental.pallas import tpu as pltpu
from jax.sharding import PartitionSpec as P

EPSILON = 1e-05
CHUNK = 256
OWN_CHUNKS = 3
NEAR_CHUNKS = 2
NEAR_ROWS = 240
FAR_ROWS = 176
FAR_FIRST = 128
CLASS_ROWS = 8


def iota(shape, axis):
    return lax.broadcasted_iota(jnp.int32, shape, axis)


def one_hot(cond):
    return jnp.where(cond, 1.0, 0.0).astype(jnp.bfloat16)


def dot(a, b):
    return jnp.dot(a, b, preferred_element_type=jnp.float32)


def dot_nt(a, b):
    return lax.dot_general(a, b, (((1,), (1,)), ((), ())), preferred_element_type=jnp.float32)


def within(index, size):
    if size & (size - 1) == 0:
        return index & (size - 1)
    return jnp.clip(index, 0, size - 1)


def wide(block):
    return jnp.concatenate([block[j : j + 1, :] for j in range(block.shape[0])], axis=1)


def normalize(total, gain, offset):
    width = total.shape[1]
    center = jnp.sum(total, axis=1, keepdims=True) / width
    centered = total - center
    spread = jnp.sum(centered * centered, axis=1, keepdims=True) / width
    return centered * lax.rsqrt(spread + EPSILON) * gain + offset


def class_plan(patches):
    starts = [0, OWN_CHUNKS] + [OWN_CHUNKS + 2 * NEAR_CHUNKS + k - 2 for k in range(2, patches - 1)]
    starts.append(OWN_CHUNKS + NEAR_CHUNKS)
    near = NEAR_CHUNKS * NEAR_ROWS
    caps = [OWN_CHUNKS * CHUNK, near] + [FAR_ROWS] * (patches - 3) + [near]
    return starts, caps, OWN_CHUNKS + 2 * NEAR_CHUNKS + patches - 3


def early_blocks(own_rows):
    return (own_rows // CHUNK * 3) // 5


def plan_edges(sizes, me, rank_me, count, recv_ref, send_ref, slot_ref, req_ref, edge_ref, send_out_ref, where_ref, slots, target, masks, position, local, totals):
    patches, ranks, mesh_rows, grid_rows, parts = sizes
    groups = recv_ref.shape[0]
    own_rows = mesh_rows // ranks
    starts, caps, chunks = class_plan(patches)
    high = slot_ref.shape[0]
    turned = slot_ref[...].astype(jnp.float32).T.astype(jnp.int32)
    for part in range(parts):
        slots[part * 128 : (part + 1) * 128, :] = ((turned >> (8 * part)) & 255).astype(jnp.float32).astype(jnp.bfloat16)

    def lookup(i, carry):
        row = wide(recv_ref[pl.ds(i * 8, 8), :])
        hot = one_hot(iota((high, 1024), 0) == (row >> 7))
        found = dot(slots[...], hot)
        low = iota((128, 1024), 0) == (row & 127)
        value = jnp.zeros((1, 1024), jnp.float32)
        for part in range(parts):
            piece = jnp.where(low, found[part * 128 : (part + 1) * 128], 0.0)
            value = value + float(256**part) * jnp.sum(piece, axis=0, keepdims=True)
        value = value.astype(jnp.int32)
        block = jnp.concatenate([value[:, j * 128 : (j + 1) * 128] for j in range(8)], axis=0)
        target[pl.ds(i * 8, 8), :] = block
        return carry

    lax.fori_loop(0, groups // 8, lookup, 0, unroll=2)

    shape = (groups, 128)
    goal = target[...]
    owner = sum((goal >= k * mesh_rows).astype(jnp.int32) for k in range(1, patches))
    inside = goal - owner * mesh_rows
    part = sum((inside >= k * own_rows).astype(jnp.int32) for k in range(1, ranks))
    offset = owner - me
    offset = jnp.where(offset < 0, offset + patches, offset)
    slot = iota(shape, 0) * 128 + iota(shape, 1)
    live = slot < count
    label = jnp.where(live, offset * ranks + part, -1)
    classes = patches * ranks
    for c in range(classes):
        masks[c * groups : (c + 1) * groups, :] = one_hot(label == c)
    early = inside - part * own_rows < early_blocks(own_rows) * CHUNK
    far = range(2 * ranks, (patches - 1) * ranks)
    for c in far:
        at = (classes + c - far[0]) * groups
        masks[at : at + groups, :] = one_hot((label == c) & early)
    steps = jnp.concatenate([one_hot(iota((128, 128), 0) <= iota((128, 128), 1)), jnp.ones((128, 128), jnp.bfloat16)], axis=1)
    size = masks.shape[0]
    for half in range(2):
        totals[half * size : (half + 1) * size, :] = dot(masks[...], steps[:, half * 128 : (half + 1) * 128])
    below = one_hot(iota((groups, groups), 1) < iota((groups, groups), 0))
    rank = jnp.zeros(shape, jnp.float32)
    over = jnp.zeros((1, 128), jnp.float32)
    for c in range(classes):
        inner = totals[c * groups : (c + 1) * groups, :]
        whole = totals[size + c * groups : size + (c + 1) * groups, :]
        before = dot(below, whole.astype(jnp.bfloat16))
        mine = jnp.where(label == c, 1.0, 0.0)
        full = before[groups - 1 :, :] + whole[groups - 1 :, :]
        spots = inner - 1.0 + before
        if c in far:
            at = (classes + c - far[0]) * groups
            ahead = totals[at : at + groups, :] + dot(below, totals[size + at : size + at + groups, :].astype(jnp.bfloat16))
            count_ahead = ahead[groups - 1 :, 127:]
            spots = jnp.where(early, ahead - 1.0, spots + count_ahead - ahead)
            over = jnp.maximum(over, jnp.where(count_ahead > float(FAR_FIRST), 1.0, 0.0))
        rank = rank + mine * spots
        over = jnp.maximum(over, jnp.where(full > float(caps[c // ranks]), 1.0, 0.0))
    rank = rank.astype(jnp.int32)
    first = jnp.zeros(shape, jnp.int32)
    cap = jnp.zeros(shape, jnp.int32)
    for k in range(patches):
        first = jnp.where(offset == k, starts[k] * CHUNK, first)
        cap = jnp.where(offset == k, caps[k], cap)
    fits = rank < cap
    near = (offset == 1) | (offset == patches - 1)
    rank = jnp.where(near & (rank >= NEAR_ROWS), rank + (CHUNK - NEAR_ROWS), rank)
    spot = part * (chunks * CHUNK) + first + rank
    spot = jnp.clip(spot, 0, ranks * chunks * CHUNK - 1)
    where_ref[...] = jnp.where(live, spot, 0)
    mine = live & (part == rank_me) & fits
    position[...] = jnp.where(mine, offset * (CLASS_ROWS * 128) + rank, -1)
    local[...] = inside - rank_me * own_rows

    rows = patches * CLASS_ROWS

    def invert(read, amount):
        def step(i, total):
            at = pl.ds(i * 8, 8)
            spots = wide(position[at, :])
            here = iota((rows, 1024), 0) == (spots >> 7)
            values = [part for value in read(i, at) for part in (value >> 8, value & 255)]
            left = jnp.concatenate(
                [jnp.where(here, value.astype(jnp.float32), 0.0).astype(jnp.bfloat16) for value in values], axis=0
            )
            right = one_hot(iota((128, 1024), 0) == (spots & 127))
            return total + dot_nt(left, right)

        total = lax.fori_loop(0, groups // 8, step, jnp.zeros((2 * amount * rows, 128), jnp.float32))
        pairs = [total[n * rows : (n + 1) * rows] for n in range(2 * amount)]
        return [(pairs[2 * n] * 256.0 + pairs[2 * n + 1]).astype(jnp.int32) for n in range(amount)]

    last = (iota((rows, 128), 0) & (CLASS_ROWS - 1)) == CLASS_ROWS - 1
    asked = invert(lambda i, at: [wide(local[at, :]) + 1], 1)[0] - 1
    req_ref[...] = jnp.where(last, over.astype(jnp.int32), asked)

    def finish():
        edge, sender = invert(
            lambda i, at: [i * 1024 + iota((1, 1024), 1), wide(send_ref[at, :]) - me * grid_rows], 2
        )
        edge_ref[...] = jnp.clip(edge, 0, groups * 128 - 1)
        send_out_ref[...] = sender

    return finish


def stage_kernel(sizes, count, receivers, senders, mesh_slot, bias_a, bias_b, gain_a, shift_a, bias_c, bias_d, gain_b, shift_b, w_edge, w_sender, w_receiver, w_edge_out, w_mesh_in, w_message_in, w_mesh_out, mesh, edge, grid, mesh_out, edge_out, flag, mesh_v, edge_v, grid_v, first_w, second_w, third_w, fourth_w, vectors, req, reqs, edges, sends, places, slots, target, masks, position, local, edge_s, where, rows_out, rows_in, results, messages, outgoing, incoming, table, gathered, staged, finished, finished_mesh, summed, local_sem, weight_send, weight_recv, req_send, req_recv, row_send, row_recv, msg_send, msg_recv, out_send, out_recv, mesh_send, mesh_recv, mesh_own):
    patches, ranks = sizes[0], sizes[1]
    me, rank = lax.axis_index("patch"), lax.axis_index("hidden")
    chunks = class_plan(patches)[2]
    far_first = OWN_CHUNKS + 2 * NEAR_CHUNKS
    full = first_w.shape[1]
    width = w_edge.shape[1]
    own_rows = mesh_v.shape[0]
    edge_rows = edge_v.shape[0]
    patch_peer = lambda k: lax.rem(me + k + patches, patches)
    rank_peer = lambda k: lax.rem(rank + k, ranks)
    side = rank + 1 - 2 * lax.rem(rank, 2)
    across = lax.rem(rank + 2, ranks)

    def class_of(chunk):
        near = (chunk - OWN_CHUNKS) // NEAR_CHUNKS
        is_near = (chunk >= OWN_CHUNKS) & (chunk < far_first)
        k = jnp.where(chunk < OWN_CHUNKS, 0, jnp.where(is_near, 1 + near * (patches - 2), chunk - far_first + 2))
        at = jnp.where(chunk < OWN_CHUNKS, chunk, jnp.where(is_near, (chunk - OWN_CHUNKS) % NEAR_CHUNKS, 0))
        return k, at

    def send(src, dst, send_sem, recv_sem, axis, peer):
        return pltpu.make_async_remote_copy(
            src_ref=src, dst_ref=dst, send_sem=send_sem, recv_sem=recv_sem,
            device_id={axis: peer}, device_id_type=pl.DeviceIdType.MESH,
        )

    weights = [
        (w_edge, first_w, 0, True),
        (w_sender, first_w, full, True),
        (w_receiver, first_w, 2 * full, True),
        (w_edge_out, second_w, 0, False),
        (w_mesh_in, third_w, 0, True),
        (w_message_in, third_w, full, True),
        (w_mesh_out, fourth_w, 0, False),
    ]
    edge_weights, mesh_weights = [7, 0, 1, 2, 3], [4, 5, 6]

    def landing(n, owner):
        if n == 7:
            return vectors.at[owner]
        _, dst, first, by_column = weights[n]
        columns = pl.ds(pl.multiple_of(owner * width, width), width)
        if by_column:
            return dst.at[pl.ds(first, full), columns]
        return dst.at[columns, :]

    def weight_copy(n, way):
        source = landing(n, across) if way == 2 else (vectors.at[rank] if n == 7 else weights[n][0])
        owner = across if way == 2 else rank
        peer = across if way == 1 else side
        return send(source, landing(n, owner), weight_send.at[way, n], weight_recv.at[way, n], "hidden", peer)

    loads = [
        pltpu.make_async_copy(mesh.at[pl.ds(pl.multiple_of(rank * own_rows, 16), own_rows)], mesh_v, local_sem.at[0]),
        pltpu.make_async_copy(edge, edge_v, local_sem.at[1]),
        pltpu.make_async_copy(grid, grid_v, local_sem.at[2]),
    ]
    for n, entry in enumerate(weights):
        loads.append(pltpu.make_async_copy(entry[0], landing(n, rank), local_sem.at[3 + n]))
    for load in loads:
        load.start()

    barrier = pltpu.get_barrier_semaphore()
    for k in range(1, patches):
        pl.semaphore_signal(barrier, inc=1, device_id={"patch": patch_peer(k)}, device_id_type=pl.DeviceIdType.MESH)
    for k in range(1, ranks):
        pl.semaphore_signal(barrier, inc=1, device_id={"hidden": rank_peer(k)}, device_id_type=pl.DeviceIdType.MESH)

    vectors[rank] = jnp.concatenate(
        [ref[...] for ref in (bias_a, bias_b, gain_a, shift_a, bias_c, bias_d, gain_b, shift_b)], axis=0
    )
    for chunk in range(OWN_CHUNKS, far_first):
        messages[chunk, NEAR_ROWS:, :] = jnp.zeros((CHUNK - NEAR_ROWS, full), jnp.bfloat16)
    for chunk in range(far_first, chunks):
        messages[chunk, FAR_ROWS:, :] = jnp.zeros((CHUNK - FAR_ROWS, full), jnp.bfloat16)

    pl.semaphore_wait(barrier, patches + ranks - 2)
    for n in edge_weights + mesh_weights:
        weight_copy(n, 1).start()
        weight_copy(n, 0).start()

    finish_plan = plan_edges(sizes, me, rank, count[0], receivers, senders, mesh_slot, req, edges, sends, places, slots, target, masks, position, local, table)

    req_copies = []
    for k in range(1, patches):
        block = pl.ds(k * CLASS_ROWS, CLASS_ROWS)
        copy = send(req.at[block], reqs.at[block], req_send.at[k], req_recv.at[k], "patch", patch_peer(k))
        copy.start()
        req_copies.append(copy)
    reqs[:CLASS_ROWS, :] = req[:CLASS_ROWS, :]
    finish_plan()
    scalars = [
        pltpu.make_async_copy(edges, edge_s, local_sem.at[10]),
        pltpu.make_async_copy(places, where, local_sem.at[11]),
    ]
    for copy in scalars:
        copy.start()

    loads[1].wait()

    @pl.loop(0, edge_rows // CHUNK)
    def _(block):
        at = pl.multiple_of(block * CHUNK, CHUNK)
        for j in range(ranks):
            table[pl.ds(j * edge_rows + at, CHUNK), :] = edge_v[pl.ds(at, CHUNK), j * width : (j + 1) * width].astype(jnp.float32)

    def columns(ref, k, at):
        turned = ref[pl.ds(pl.multiple_of(k * CLASS_ROWS, CLASS_ROWS), CLASS_ROWS), :].astype(jnp.float32).T
        lane = iota(turned.shape, 1)
        picks = [jnp.sum(jnp.where(lane == 2 * at + n, turned, 0.0), axis=1, keepdims=True) for n in range(2)]
        return jnp.concatenate(picks, axis=0).astype(jnp.int32)

    def pick(column, source, step):
        total = None
        for first in range(0, source.shape[0], step):
            hot = one_hot(iota((column.shape[0], step), 1) == column - first)
            piece = dot(hot, source[first : first + step, :])
            total = piece if total is None else total + piece
        return total.astype(jnp.bfloat16)

    def row_copy(chunk, k, rows):
        part = pl.ds(0, rows)
        return send(
            rows_out.at[chunk, part], rows_in.at[chunk, part], row_send.at[chunk], row_recv.at[chunk], "patch", patch_peer(-k)
        )

    def msg_copy(chunk, k, rows, late=False):
        part = pl.ds(FAR_FIRST, rows - FAR_FIRST) if late else pl.ds(0, FAR_FIRST if rows == FAR_ROWS else rows)
        n = 1 if late else 0
        return send(
            results.at[chunk, part], messages.at[chunk, part], msg_send.at[n, chunk], msg_recv.at[n, chunk], "patch", patch_peer(k)
        )

    def out_copy(chunk, k, rows):
        peer, part = rank_peer(k), pl.ds(0, rows)
        return send(
            outgoing.at[peer, chunk, part], incoming.at[rank, chunk, part],
            out_send.at[k, chunk], out_recv.at[k, chunk], "hidden", peer,
        )

    loads[0].wait()
    gather_step = own_rows if own_rows <= 1280 else CHUNK
    for copy in req_copies:
        copy.wait_recv()

    def serve(chunk, rows):
        k, at = class_of(chunk)
        rows_out[chunk, :rows, :] = pick(columns(reqs, k, at)[:rows], mesh_v, gather_step)
        row_copy(chunk, k, rows).start()

    far_count, near_count = chunks - far_first, far_first - OWN_CHUNKS

    def in_turn(act):
        @pl.loop(0, max(far_count, near_count))
        def _(j):
            @pl.when(j < far_count)
            def _():
                act(far_first + j, FAR_ROWS)

            @pl.when(j < near_count)
            def _():
                act(OWN_CHUNKS + j, NEAR_ROWS)

    in_turn(serve)

    loads[2].wait()
    for copy in scalars:
        copy.wait()
    for load in loads[3:]:
        load.wait()
    for n in edge_weights:
        weight_copy(n, 1).wait_recv()
        weight_copy(n, 2).start()

    @pl.loop(0, OWN_CHUNKS)
    def _(chunk):
        rows_in[chunk] = pick(columns(reqs, 0, chunk), mesh_v, gather_step)

    for n in edge_weights:
        weight_copy(n, 0).wait_recv()
        weight_copy(n, 2).wait_recv()

    def vector_row(n):
        return jnp.concatenate([vectors[j, n : n + 1, :] for j in range(ranks)], axis=1)

    def collect(line, first, amount):
        for n in range(amount):
            spot = within(edge_s[line, n], edge_rows)
            for j in range(ranks):
                gathered[j, pl.ds(first + n, 1), :] = table[pl.ds(j * edge_rows + spot, 1), :]

    def edge_stage(chunk, rows):
        k, at = class_of(chunk)
        @pl.loop(0, 2)
        def _(half):
            collect(k * CLASS_ROWS + 2 * at + half, pl.multiple_of(half * 128, 128), 128)
        own_edge = jnp.concatenate([gathered[j, :rows, :] for j in range(ranks)], axis=1)
        pre = dot(own_edge.astype(jnp.bfloat16), first_w[:full, :])
        sender = pick(columns(sends, k, at)[:rows], grid_v, 1024)
        pre = pre + dot(sender, first_w[full : 2 * full, :])
        return own_edge, pre

    def edge_finish(chunk, rows, own_edge, pre):
        pre = pre + dot(rows_in[chunk, :rows, :], first_w[2 * full :, :]) + vector_row(0)
        hidden = jax.nn.silu(pre).astype(jnp.bfloat16)
        total = dot(hidden, second_w[...]) + vector_row(1)
        message = normalize(total, vector_row(2), vector_row(3))
        result = (own_edge + message).astype(jnp.bfloat16)
        for j in range(ranks):
            outgoing[j, chunk, :rows, :] = result[:, j * width : (j + 1) * width]
        return message.astype(jnp.bfloat16)

    def remote_chunk(chunk, rows):
        k, _ = class_of(chunk)
        own_edge, pre = edge_stage(chunk, rows)
        row_copy(chunk, k, rows).wait_recv()
        results[chunk, :rows, :] = edge_finish(chunk, rows, own_edge, pre)
        msg_copy(chunk, k, rows).start()
        for j in range(1, ranks):
            out_copy(chunk, j, rows).start()

    @pl.loop(0, OWN_CHUNKS)
    def _(chunk):
        own_edge, pre = edge_stage(chunk, CHUNK)
        messages[chunk] = edge_finish(chunk, CHUNK, own_edge, pre)
        for j in range(1, ranks):
            out_copy(chunk, j, CHUNK).start()

    in_turn(remote_chunk)

    @pl.loop(far_first, chunks)
    def _(chunk):
        msg_copy(chunk, class_of(chunk)[0], FAR_ROWS, True).start()

    for n in mesh_weights:
        weight_copy(n, 1).wait_recv()
        weight_copy(n, 2).start()

    def each_chunk(act):
        @pl.loop(0, OWN_CHUNKS)
        def _(chunk):
            act(chunk, CHUNK, False)

        @pl.loop(OWN_CHUNKS, far_first)
        def _(chunk):
            act(chunk, NEAR_ROWS, True)

        @pl.loop(far_first, chunks)
        def _(chunk):
            act(chunk, FAR_ROWS, True)

    def await_out(chunk, rows, remote):
        for j in range(1, ranks):
            out_copy(chunk, j, rows).wait_recv()

    blocks = own_rows // CHUNK

    def await_message(chunk, rows):
        msg_copy(chunk, class_of(chunk)[0], rows).wait_recv()

    def add_messages(chunk, first=0, last=blocks, depth=CHUNK):
        k, at = class_of(chunk)
        row = pl.multiple_of(k * CLASS_ROWS, CLASS_ROWS)
        asked = reqs[pl.ds(row, CLASS_ROWS), :]
        line = iota(asked.shape, 0)
        pair = [jnp.sum(jnp.where(line == 2 * at + n, asked, 0), axis=0, keepdims=True) for n in range(2)]
        wanted = jnp.concatenate(pair, axis=1)
        for block in range(first, last):
            span = slice(block * CHUNK, (block + 1) * CHUNK)
            hot = one_hot(iota((CHUNK, depth), 0) + block * CHUNK == wanted[:, :depth])
            summed[span, :] += dot(hot, messages[chunk, :depth, :])

    summed[...] = jnp.zeros(summed.shape, jnp.float32)

    @pl.loop(0, OWN_CHUNKS)
    def _(chunk):
        add_messages(chunk)

    for n in mesh_weights:
        weight_copy(n, 0).wait_recv()
        weight_copy(n, 2).wait_recv()

    def mesh_copy(block, k):
        peer = rank_peer(k)
        at = pl.ds(pl.multiple_of(rank * own_rows + block * CHUNK, CHUNK), CHUNK)
        return send(
            finished_mesh.at[peer, pl.ds(pl.multiple_of(block * CHUNK, CHUNK), CHUNK)], mesh_out.at[at],
            mesh_send.at[k, block], mesh_recv.at[k, block], "hidden", peer,
        )

    def mesh_local(block):
        at = pl.ds(pl.multiple_of(rank * own_rows + block * CHUNK, CHUNK), CHUNK)
        return pltpu.make_async_copy(
            finished_mesh.at[rank, pl.ds(pl.multiple_of(block * CHUNK, CHUNK), CHUNK)], mesh_out.at[at], mesh_own.at[block]
        )

    @pl.loop(0, far_count + near_count)
    def _(j):
        paired = 2 * min(far_count, near_count)
        odd = lax.rem(j, 2)
        rest = (far_first if far_count > near_count else OWN_CHUNKS) + j - paired // 2
        chunk = jnp.where(j < paired, jnp.where(odd == 0, far_first, OWN_CHUNKS) + j // 2, rest)

        @pl.when(chunk >= far_first)
        def _():
            await_message(chunk, FAR_ROWS)
            add_messages(chunk, 0, early_blocks(own_rows), FAR_FIRST)

        @pl.when(chunk < far_first)
        def _():
            await_message(chunk, NEAR_ROWS)
            add_messages(chunk)

    @pl.loop(0, blocks)
    def _(block):
        @pl.when(block == early_blocks(own_rows))
        def _():
            @pl.loop(far_first, chunks)
            def _(chunk):
                msg_copy(chunk, class_of(chunk)[0], FAR_ROWS, True).wait_recv()
                add_messages(chunk, early_blocks(own_rows), blocks)

        at = pl.ds(pl.multiple_of(block * CHUNK, CHUNK), CHUNK)
        own = mesh_v[at, :]
        pre = dot(own, third_w[:full, :]) + dot(summed[at, :].astype(jnp.bfloat16), third_w[full:, :]) + vector_row(4)
        hidden = jax.nn.silu(pre).astype(jnp.bfloat16)
        total = dot(hidden, fourth_w[...]) + vector_row(5)
        update = normalize(total, vector_row(6), vector_row(7))
        result = (own.astype(jnp.float32) + update).astype(jnp.bfloat16)
        for j in range(ranks):
            finished_mesh[j, at, :] = result[:, j * width : (j + 1) * width]
        for k in range(1, ranks):
            mesh_copy(block, k).start()
        mesh_local(block).start()

    each_chunk(await_out)

    @pl.loop(0, ranks)
    def _(j):
        @pl.when(j == rank)
        def _():
            @pl.loop(0, chunks)
            def _(chunk):
                table[pl.ds(pl.multiple_of((j * chunks + chunk) * CHUNK, CHUNK), CHUNK), :] = outgoing[j, chunk].astype(jnp.float32)

        @pl.when(j != rank)
        def _():
            @pl.loop(0, chunks)
            def _(chunk):
                table[pl.ds(pl.multiple_of((j * chunks + chunk) * CHUNK, CHUNK), CHUNK), :] = incoming[j, chunk].astype(jnp.float32)

    own_columns = pl.ds(pl.multiple_of(rank * width, width), width)

    @pl.loop(0, edge_rows // 128)
    def _(line):
        for n in range(128):
            spot = within(where[line, n], table.shape[0])
            staged[n : n + 1, :] = table[pl.ds(spot, 1), :]
        at = pl.ds(pl.multiple_of(line * 128, 128), 128)
        live = iota((128, width), 0) + line * 128 < count[0]
        finished[at, :] = jnp.where(live, staged[...], edge_v[at, own_columns].astype(jnp.float32)).astype(jnp.bfloat16)

    last = pltpu.make_async_copy(finished, edge_out, local_sem.at[0])
    last.start()

    over = reqs[CLASS_ROWS - 1 : CLASS_ROWS, :]
    for k in range(1, patches):
        row = (k + 1) * CLASS_ROWS - 1
        over = jnp.maximum(over, reqs[row : row + 1, :])
    flag[0] = jnp.max(over)

    for copy in req_copies:
        copy.wait_send()
    for way in range(3):
        for n in edge_weights + mesh_weights:
            weight_copy(n, way).wait_send()

    def drain(chunk, rows, remote):
        for j in range(1, ranks):
            out_copy(chunk, j, rows).wait_send()
        if remote:
            k = class_of(chunk)[0]
            row_copy(chunk, k, rows).wait_send()
            msg_copy(chunk, k, rows).wait_send()
            if rows == FAR_ROWS:
                msg_copy(chunk, k, rows, True).wait_send()

    each_chunk(drain)

    @pl.loop(0, blocks)
    def _(block):
        for k in range(1, ranks):
            mesh_copy(block, k).wait()
        mesh_local(block).wait()

    last.wait()


def run_stages(patches, ranks, count, receivers, senders, mesh_slot, vectors, weights, mesh_latent, edge_latent, grid_latent):
    full, width = weights[0].shape
    mesh_rows, edge_rows, grid_rows = mesh_latent.shape[0], edge_latent.shape[0], grid_latent.shape[0]
    own_rows = mesh_rows // ranks
    chunks = class_plan(patches)[2]
    groups, high = edge_rows // 128, mesh_slot.shape[0] // 128
    parts = 1
    while 256**parts < mesh_slot.shape[0]:
        parts += 1
    bf16, f32, i32 = jnp.bfloat16, jnp.float32, jnp.int32
    dma = pltpu.SemaphoreType.DMA
    vmem = pl.BlockSpec(memory_space=pltpu.VMEM)
    smem = pl.BlockSpec(memory_space=pltpu.SMEM)
    hbm = pl.BlockSpec(memory_space=pl.ANY)
    blocks = own_rows // CHUNK
    lists = patches * CLASS_ROWS
    classes = (patches + patches - 3) * ranks * groups
    return pl.pallas_call(
        functools.partial(stage_kernel, (patches, ranks, mesh_rows, grid_rows, parts)),
        in_specs=[smem] + [vmem] * 11 + [hbm] * 10,
        out_specs=[hbm, hbm, smem],
        out_shape=[
            jax.ShapeDtypeStruct((mesh_rows, width), bf16),
            jax.ShapeDtypeStruct((edge_rows, width), bf16),
            jax.ShapeDtypeStruct((1,), i32),
        ],
        scratch_shapes=[
            pltpu.VMEM((own_rows, full), bf16),
            pltpu.VMEM((edge_rows, full), bf16),
            pltpu.VMEM((grid_rows, full), bf16),
            pltpu.VMEM((3 * full, full), bf16),
            pltpu.VMEM((full, full), bf16),
            pltpu.VMEM((2 * full, full), bf16),
            pltpu.VMEM((full, full), bf16),
            pltpu.VMEM((ranks, 8, width), f32),
            pltpu.VMEM((lists, 128), i32),
            pltpu.VMEM((lists, 128), i32),
            pltpu.VMEM((lists, 128), i32),
            pltpu.VMEM((lists, 128), i32),
            pltpu.VMEM((groups, 128), i32),
            pltpu.VMEM((parts * 128, high), bf16),
            pltpu.VMEM((groups, 128), i32),
            pltpu.VMEM((classes, 128), bf16),
            pltpu.VMEM((groups, 128), i32),
            pltpu.VMEM((groups, 128), i32),
            pltpu.SMEM((lists, 128), i32),
            pltpu.SMEM((groups, 128), i32),
            pltpu.VMEM((chunks, CHUNK, full), bf16),
            pltpu.VMEM((chunks, CHUNK, full), bf16),
            pltpu.VMEM((chunks, CHUNK, full), bf16),
            pltpu.VMEM((chunks, CHUNK, full), bf16),
            pltpu.VMEM((ranks, chunks, CHUNK, width), bf16),
            pltpu.VMEM((ranks, chunks, CHUNK, width), bf16),
            pltpu.VMEM((ranks * max(edge_rows, chunks * CHUNK), width), f32),
            pltpu.VMEM((ranks, CHUNK, width), f32),
            pltpu.VMEM((128, width), f32),
            pltpu.VMEM((edge_rows, width), bf16),
            pltpu.VMEM((ranks, own_rows, width), bf16),
            pltpu.VMEM((own_rows, full), f32),
            dma((12,)),
            dma((3, 8)),
            dma((3, 8)),
            dma((patches,)),
            dma((patches,)),
            dma((chunks,)),
            dma((chunks,)),
            dma((2, chunks)),
            dma((2, chunks)),
            dma((ranks, chunks)),
            dma((ranks, chunks)),
            dma((ranks, blocks)),
            dma((ranks, blocks)),
            dma((blocks,)),
        ],
        compiler_params=pltpu.CompilerParams(
            collective_id=0, has_side_effects=True, vmem_limit_bytes=67043328
        ),
        name="run_stages",
    )(
        count, receivers.reshape(groups, 128), senders.reshape(groups, 128), mesh_slot.reshape(high, 128),
        *[vector[None] for vector in vectors], *weights, mesh_latent, edge_latent, grid_latent,
    )


def pieces(x, axis, size):
    return [x] + [lax.ppermute(x, axis, [((j + k) % size, j) for j in range(size)]) for k in range(1, size)]


def rows_at(x, index):
    return x.at[index].get(mode="promise_in_bounds")


def dense(patches, ranks, operands):
    (grid_latent, mesh_latent, edge_latent, senders, receivers, mesh_slot, edge_counts, w_edge, w_sender, w_receiver,
     edge_bias, w_edge_out, edge_out_bias, edge_gain, edge_shift, w_mesh_in, w_message_in, mesh_bias, w_mesh_out,
     mesh_out_bias, mesh_gain, mesh_shift) = operands
    me, rank = lax.axis_index("patch"), lax.axis_index("hidden")
    mesh_rows, edge_rows = mesh_latent.shape[0], edge_latent.shape[0]
    mesh_total = mesh_slot.shape[0]
    width = w_edge.shape[1]
    bf16 = jnp.bfloat16

    def own(x):
        return lax.dynamic_slice_in_dim(x, rank * width, width, 1)

    def turn(x, axis):
        full = jnp.concatenate(pieces(x, "hidden", ranks), axis)
        return full

    def natural(x):
        full = turn(x, 0)
        return jnp.roll(full, rank * width, 0)[None]

    def spread_mlp(pre, w_out, bias, gain, shift):
        w_full, bias_full = turn(w_out, 0), natural(bias)
        step = CHUNK if pre.shape[0] % CHUNK == 0 else pre.shape[0]

        def block(i, result):
            part = lax.dynamic_slice_in_dim(pre, i * step, step, 0)
            hidden = turn(jax.nn.silu(part).astype(bf16), 1)
            total = dot(hidden, w_full) + bias_full
            center = jnp.mean(total, axis=1, keepdims=True)
            centered = total - center
            scale = lax.rsqrt(jnp.mean(centered * centered, axis=1, keepdims=True) + EPSILON)
            update = own(centered * scale) * gain[None] + shift[None]
            return lax.dynamic_update_slice_in_dim(result, update, i * step, 0)

        return lax.fori_loop(0, pre.shape[0] // step, block, jnp.zeros(pre.shape, jnp.float32))

    table = jnp.concatenate(pieces(dot(mesh_latent, w_receiver).astype(bf16), "patch", patches), 0)
    target = lax.rem(rows_at(mesh_slot, receivers) + (mesh_total - me * mesh_rows), mesh_total)
    sent = rows_at(dot(grid_latent, w_sender), senders - me * grid_latent.shape[0])
    pre = dot(edge_latent, w_edge) + sent + rows_at(table, target).astype(jnp.float32) + edge_bias[None]
    message = spread_mlp(pre, w_edge_out, edge_out_bias, edge_gain, edge_shift)
    live = jnp.arange(edge_rows)[:, None] < edge_counts[0]
    message = jnp.where(live, message, 0.0)
    edge_out = (own(edge_latent).astype(jnp.float32) + message).astype(bf16)
    rounded = message.astype(bf16)

    def add_block(i, sums):
        hot = (target[None] == (i * CHUNK + jnp.arange(CHUNK))[:, None]).astype(bf16)
        return lax.dynamic_update_slice_in_dim(sums, dot(hot, rounded), i * CHUNK, 0)

    sums = jnp.zeros((mesh_total, width), jnp.float32)
    if mesh_total % CHUNK:
        sums = sums.at[target].add(message, mode="promise_in_bounds")
    else:
        sums = lax.fori_loop(0, mesh_total // CHUNK, add_block, sums)
    summed = sums[:mesh_rows]
    for k in range(1, patches):
        part = sums[k * mesh_rows : (k + 1) * mesh_rows].astype(bf16)
        part = lax.ppermute(part, "patch", [(j, (j + k) % patches) for j in range(patches)])
        summed = summed + part.astype(jnp.float32)
    turned = jnp.roll(w_message_in, -rank * width, 0)
    pre = dot(mesh_latent, w_mesh_in) + dot(turn(summed.astype(bf16), 1), turned) + mesh_bias[None]
    update = spread_mlp(pre, w_mesh_out, mesh_out_bias, mesh_gain, mesh_shift)
    mesh_out = (own(mesh_latent).astype(jnp.float32) + update).astype(bf16)
    return mesh_out, edge_out


def shards(patches, ranks, *operands):
    (grid_latent, mesh_latent, edge_latent, senders, receivers, mesh_slot, edge_counts, w_edge, w_sender, w_receiver,
     edge_bias, w_edge_out, edge_out_bias, edge_gain, edge_shift, w_mesh_in, w_message_in, mesh_bias, w_mesh_out,
     mesh_out_bias, mesh_gain, mesh_shift) = operands
    mesh_rows, edge_rows, grid_rows = mesh_latent.shape[0], edge_latent.shape[0], grid_latent.shape[0]
    fits = (
        w_edge.shape[1] % 128 == 0
        and ranks == 4
        and 4 < patches <= 16
        and edge_rows % 1024 == 0
        and grid_rows % 1024 == 0
        and mesh_rows % (ranks * CHUNK) == 0
        and mesh_slot.shape[0] % 1024 == 0
    )
    if not fits:
        return dense(patches, ranks, operands)
    vectors = (edge_bias, edge_out_bias, edge_gain, edge_shift, mesh_bias, mesh_out_bias, mesh_gain, mesh_shift)
    weights = (w_edge, w_sender, w_receiver, w_edge_out, w_mesh_in, w_message_in, w_mesh_out)
    mesh_out, edge_out, flag = run_stages(
        patches, ranks, edge_counts, receivers, senders, mesh_slot, vectors, weights, mesh_latent, edge_latent, grid_latent
    )
    return lax.cond(
        flag[0] > 0,
        lambda outs, args: dense(patches, ranks, args),
        lambda outs, args: outs,
        (mesh_out, edge_out),
        operands,
    )


def solution(mesh):
    columns, rows, line, patch = P(None, "hidden"), P("hidden", None), P("hidden"), P("patch", None)
    return jax.shard_map(
        functools.partial(shards, mesh.shape["patch"], mesh.shape["hidden"]),
        mesh=mesh,
        in_specs=(
            patch, patch, patch, P("patch"), P("patch"), P(), P("patch"),
            columns, columns, columns, line, rows, line, line, line,
            columns, columns, line, rows, line, line, line,
        ),
        out_specs=(P("patch", "hidden"), P("patch", "hidden")),
        check_vma=False,
    )
```
